256 devices in a mesh: dp: 16 (over y, x_lo, core), fsdp: 16 (over z, x_hi).
Axes of the slice: x: 4 (x_hi: 2, x_lo: 2; x = x_hi * 2 + x_lo), y: 4, z: 8, core: 2. Of those that a mesh axis runs over, the one named last changes fastest.
Arguments:
- tokens: bfloat16 [2048, 5120], P('dp'), may hold values from -6 to 6
- targets: bfloat16 [2048, 5120], P('dp'), may hold values from -12 to 12
- norm_gain: float32 [5120], replicated, may hold values from 0.5 to 1.5
- up_master: float32 [5120, 6912], P('dp', 'fsdp'), may hold values from -0.078125 to 0.078125
- down_master: float32 [6912, 5120], P('fsdp', 'dp'), may hold values from -0.078125 to 0.078125
- up_probe: int32 [160, 6912], P(None, 'fsdp'), may hold values from -2147483648 to 2147483646
- down_probe: int32 [6912, 160], P('fsdp'), may hold values from -2147483648 to 2147483646
- up_first: float32 [5120, 6912], P('dp', 'fsdp'), may hold values from -0.012 to 0.012
- up_second: float32 [5120, 6912], P('dp', 'fsdp'), may hold values from 0.0001 to 0.001
- down_first: float32 [6912, 5120], P('fsdp', 'dp'), may hold values from -0.012 to 0.012
- down_second: float32 [6912, 5120], P('fsdp', 'dp'), may hold values from 0.0001 to 0.001
Outputs:
- loss: float32 [], replicated
- up_moment: float32 [5120, 6912], P('dp', 'fsdp')
- up_curvature: float32 [5120, 6912], P('dp', 'fsdp')
- up_step: float32 [5120, 6912], P('dp', 'fsdp')
- down_moment: float32 [6912, 5120], P('fsdp', 'dp')
- down_curvature: float32 [6912, 5120], P('fsdp', 'dp')
- down_step: float32 [6912, 5120], P('fsdp', 'dp')
The draws below stay inside these ranges and needn't reach their ends.
Inputs may be any that keep to these rules, and one draw needn't show every extreme that they name: `up_probe`: any 32-bit word; each bit gives one probe sign. `down_probe`: any 32-bit word; each bit gives one probe sign.
All inputs are finite; a program needn't handle non-finite values.
Results may differ from the reference program's by a relative error of at most 0.03.
Values may be sent and summed in bfloat16 or wider, within the bound.
No kernel may reach another device: no remote copies, remote signals or barrier semaphores. Data moves between devices by JAX's collectives and lax.ppermute only.
A program may use at most 128 MiB of HBM per device.

```python
import math
import jax
import jax.numpy as jnp
from jax import lax

D = 5120
FF = 6912
TOK_DEV = 128
BLOCK = 16
STEP = 10
TOKENS = 2048
N_DP = 16


def draw_targets(key, part):
    rows = jnp.arange(TOKENS, dtype=jnp.float32)[:, None]
    ratio = rows / jnp.float32(max(TOKENS - 1, 1))
    scale = jnp.exp(ratio * jnp.log(jnp.float32(3.0)))
    base = jnp.clip(jax.random.normal(key, (TOKENS, D), jnp.float32), -4.0, 4.0)
    return (base * scale).astype(jnp.bfloat16)


def with_ends(entries, own_key, low, largest):
    extent = entries.shape
    place = [jax.random.randint(jax.random.fold_in(own_key, axis), (), 0, extent[axis]) for axis in range(len(extent))]
    entries = entries.at[tuple(place)].set(low)
    longest = extent.index(max(extent))
    place[longest] = (place[longest] + 1) % extent[longest]
    return entries.at[tuple(place)].set(largest)


def with_spikes(values, stream_key, source, target, blocks, factor):
    def block_of(axis_at):
        return (jnp.arange(values.shape[axis_at]) // (values.shape[axis_at] // blocks)).reshape((-1,) + (1,) * (values.ndim - 1 - axis_at))

    near = jax.random.permutation(stream_key, blocks)[block_of(target)]
    second = (block_of(target) + blocks // 2) % blocks
    return jnp.where((block_of(source) == near) | (block_of(source) == second), factor * values, values)


def block_scale(key, shape, shards, low, top_value):
    def one(axis_at, blocks):
        heights = jax.random.uniform(jax.random.fold_in(jax.random.fold_in(key, 6), axis_at), (blocks,), jnp.float32, low / len(shards), top_value / len(shards))
        return jnp.repeat(jnp.exp(heights), shape[axis_at] // blocks).reshape((-1,) + (1,) * (len(shape) - axis_at - 1))

    level = one(*shards[0])
    for cut in shards[1:]:
        level = level * one(*cut)
    return level


def gaussian(own_key, extent, scale, bound, split=(), held_as=jnp.bfloat16):
    drawn = jax.random.normal(own_key, extent, jnp.float32) * scale
    if len(split) > 0:
        drawn = block_scale(own_key, extent, split, -0.22, 0.18) * drawn
    return jnp.clip(drawn, min=-bound, max=bound).astype(held_as)


def gaussian_with(stream_key, dims, width, limit, split, heavy, kind=jnp.bfloat16):
    drawn = width * jax.random.normal(stream_key, dims, jnp.float32)
    if split:
        drawn = drawn * block_scale(stream_key, dims, split, -0.22, 0.18)
    return jnp.clip(with_spikes(drawn, jax.random.fold_in(stream_key, 3), *heavy), -limit, limit).astype(kind)


def setup_inputs(seed: int = 0) -> dict:
    splits = jax.random.split(jax.random.key(seed), 12)
    tokens = gaussian_with(splits[0], (TOKENS, D), 1.0, 6.0, ((0, 16),), (0, 1, 16, 2.0))
    targets = draw_targets(jax.random.fold_in(splits[11], 71), 0)
    norm_gain = jnp.clip(1.0 + 0.1 * jax.random.normal(splits[2], (D,), jnp.float32), 0.5, 1.5)
    up_master = gaussian(splits[3], (D, FF), D ** -0.5, 0.078125, ((0, 16), (1, 16)), jnp.float32)
    down_master = gaussian(splits[4], (FF, D), FF ** -0.5, 0.078125, ((0, 16), (1, 16)), jnp.float32)
    up_probe = with_ends(jax.random.randint(splits[5], (D // 32, FF), -2147483648, 2147483647), jax.random.fold_in(splits[5], 1), -2147483648, 2147483646).astype(jnp.int32)
    down_probe = with_ends(jax.random.randint(splits[6], (FF, D // 32), -2147483648, 2147483647), jax.random.fold_in(splits[6], 1), -2147483648, 2147483646).astype(jnp.int32)
    up_first = gaussian(splits[7], (D, FF), 0.002, 0.012, ((0, 16), (1, 16)), jnp.float32)
    up_second = jnp.clip(jnp.exp(math.log(0.001) - 2.3025852 * jax.random.uniform(splits[8], (D, FF), jnp.float32) ** block_scale(splits[8], (D, FF), ((0, 16), (1, 16)), -0.2, 0.2)), 0.0001, 0.001)
    down_first = gaussian(splits[9], (FF, D), 0.002, 0.012, ((0, 16), (1, 16)), jnp.float32)
    down_second = jnp.clip(jnp.exp(math.log(0.001) - 2.3025852 * jax.random.uniform(splits[10], (FF, D), jnp.float32) ** block_scale(splits[10], (FF, D), ((0, 16), (1, 16)), -0.2, 0.2)), 0.0001, 0.001)
    return dict(tokens=tokens, targets=targets, norm_gain=norm_gain, up_master=up_master, down_master=down_master, up_probe=up_probe, down_probe=down_probe, up_first=up_first, up_second=up_second, down_first=down_first, down_second=down_second)


norm_eps = 1e-05
beta_one = 0.9
beta_two = 0.999
adam_eps = 1e-08

def signs_rows(probe):
    shifts = jnp.arange(32, dtype=jnp.int32)[:, None, None]
    bits = jnp.bitwise_and(jnp.right_shift(probe[None, :, :], shifts), 1)
    return (1 - 2 * bits).reshape(32 * probe.shape[0], probe.shape[1]).astype(jnp.bfloat16)

def signs_cols(probe):
    shifts = jnp.arange(32, dtype=jnp.int32)[None, :, None]
    bits = jnp.bitwise_and(jnp.right_shift(probe[:, None, :], shifts), 1)
    return (1 - 2 * bits).reshape(probe.shape[0], 32 * probe.shape[1]).astype(jnp.bfloat16)

def dot_first(left, right):
    return lax.dot_general(left, right, (((0,), (0,)), ((), ())), preferred_element_type=jnp.float32)

def dot_last(left, right):
    return lax.dot_general(left, right, (((1,), (1,)), ((), ())), preferred_element_type=jnp.float32)

def rounded(value):
    return lax.optimization_barrier(value.astype(jnp.bfloat16)).astype(jnp.float32)

def block_pass(rows, goal, norm_gain, up_weight, down_weight, up_signs, down_signs, tokens_all):
    values = rows.astype(jnp.float32)
    scale = lax.rsqrt(lax.optimization_barrier(jnp.mean(values * values, axis=-1, keepdims=True)) + norm_eps)
    normed = (values * scale * norm_gain).astype(jnp.bfloat16)
    preact = jnp.dot(normed, up_weight, preferred_element_type=jnp.float32)
    logistic = jax.nn.sigmoid(preact)
    active = (preact * logistic).astype(jnp.bfloat16)
    slopes = logistic * (1.0 + preact * (1.0 - logistic))
    curves = logistic * (1.0 - logistic) * (2.0 + preact * (1.0 - 2.0 * logistic))
    preact_dir = jnp.dot(normed, up_signs, preferred_element_type=jnp.float32)
    active_dir = (slopes * preact_dir).astype(jnp.bfloat16)
    output = jnp.dot(active, down_weight, preferred_element_type=jnp.float32)
    output_dir = jnp.dot(active_dir, down_weight, preferred_element_type=jnp.float32) + jnp.dot(active, down_signs, preferred_element_type=jnp.float32)
    diff = output - goal.astype(jnp.float32)
    residual = (diff / tokens_all).astype(jnp.bfloat16)
    residual_dir = (output_dir / tokens_all).astype(jnp.bfloat16)
    loss_part = 0.5 * jnp.sum(diff * diff) / tokens_all
    grad_active = dot_last(residual, down_weight)
    hess_active = dot_last(residual_dir, down_weight) + dot_last(residual, down_signs)
    grad_preact = (slopes * grad_active).astype(jnp.bfloat16)
    hess_preact = (curves * preact_dir * grad_active + slopes * hess_active).astype(jnp.bfloat16)
    up_grad = rounded(dot_first(normed, grad_preact))
    up_hess = rounded(dot_first(normed, hess_preact))
    down_grad = rounded(dot_first(active, residual))
    down_hess = rounded(dot_first(active, residual_dir) + dot_first(active_dir, residual))
    return (up_grad, up_hess, down_grad, down_hess, loss_part)

def moments(grad, hess, signs, first, second):
    hut = jnp.abs(signs.astype(jnp.float32) * hess)
    rows, cols = hut.shape
    means = lax.optimization_barrier(jnp.mean(hut.reshape(rows, cols // BLOCK, BLOCK), axis=-1))
    diag = jnp.repeat(means, BLOCK, axis=1)
    first_new = beta_one * first + (1.0 - beta_one) * grad
    second_new = beta_two * second + (1.0 - beta_two) * diag * diag
    direction = first_new / (1.0 - beta_one ** STEP) / (jnp.sqrt(second_new / (1.0 - beta_two ** STEP)) + adam_eps)
    return (first_new, second_new, direction)

def reference(tokens, targets, norm_gain, up_master, down_master, up_probe, down_probe, up_first, up_second, down_first, down_second):
    up_weight = up_master.astype(jnp.bfloat16)
    down_weight = down_master.astype(jnp.bfloat16)
    up_signs = signs_rows(up_probe)
    down_signs = signs_cols(down_probe)
    tokens_all = jnp.float32(TOKENS)
    blocks_in = tokens.reshape(N_DP, TOK_DEV, D)
    blocks_goal = targets.reshape(N_DP, TOK_DEV, D)

    def visit(carry, block):
        terms = block_pass(block[0], block[1], norm_gain, up_weight, down_weight, up_signs, down_signs, tokens_all)
        return (tuple((c + t for c, t in zip(carry, terms))), None)
    start = (jnp.zeros((D, FF), jnp.float32), jnp.zeros((D, FF), jnp.float32), jnp.zeros((FF, D), jnp.float32), jnp.zeros((FF, D), jnp.float32), jnp.zeros((), jnp.float32))
    totals, _ = lax.scan(visit, start, (blocks_in, blocks_goal))
    up_grad, up_hess, down_grad, down_hess, loss = totals
    up_moment, up_curvature, up_step = moments(up_grad, up_hess, up_signs, up_first, up_second)
    down_moment, down_curvature, down_step = moments(down_grad, down_hess, down_signs, down_first, down_second)
    return (loss, up_moment, up_curvature, up_step, down_moment, down_curvature, down_step)
```

```python
import jax
import jax.numpy as jnp
from jax import lax
from jax.sharding import Mesh, PartitionSpec as P

BLOCK = 16
STEP = 10
N_Z = 8

norm_eps = 1e-05
beta_one = 0.9
beta_two = 0.999
adam_eps = 1e-08

DP = ("y", "xlo", "core")
FS = ("z", "xhi")


def signs_rows(probe):
    shifts = jnp.arange(32, dtype=jnp.int32)[:, None, None]
    bits = jnp.bitwise_and(jnp.right_shift(probe[None, :, :], shifts), 1)
    return (1 - 2 * bits).reshape(32 * probe.shape[0], probe.shape[1]).astype(jnp.bfloat16)


def own_signs(probe, index):
    shifts = (2 * index + jnp.arange(2, dtype=jnp.int32))[:, None, None]
    bits = jnp.bitwise_and(jnp.right_shift(probe[None, :, :], shifts), 1)
    return (1 - 2 * bits).reshape(2 * probe.shape[0], probe.shape[1]).astype(jnp.float32)


def dot_last(left, right):
    return lax.dot_general(
        left, right, (((1,), (1,)), ((), ())), preferred_element_type=jnp.float32
    )


def dot_plain(left, right):
    return jnp.dot(left, right, preferred_element_type=jnp.float32)


def dot_first(left, right):
    return lax.dot_general(
        left, right, (((0,), (0,)), ((), ())), preferred_element_type=jnp.float32
    )


def gathered(shard, axis):
    return lax.all_gather(shard, axis, axis=0, tiled=True)


def sent_to_all(shard, axis):
    devices = lax.axis_size(axis)
    return lax.all_to_all(
        jnp.broadcast_to(shard[None], (devices, *shard.shape)), axis, 0, 0, tiled=True
    )


def after(value, other):
    return lax.optimization_barrier((value, other))[0]


def interleaved(first, second):
    rows, cols = first.shape
    parts = [v.reshape(N_Z, rows // N_Z, cols) for v in (first, second)]
    return jnp.stack(parts, axis=1).reshape(2 * rows, cols)


def apart(both):
    rows, cols = both.shape
    parts = both.reshape(N_Z, 2, rows // (2 * N_Z), cols)
    return parts[:, 0].reshape(rows // 2, cols), parts[:, 1].reshape(rows // 2, cols)


def over_pairs(value):
    total = value
    for axis, pairs in (
        ("core", ((0, 1), (1, 0))),
        ("xlo", ((0, 1), (1, 0))),
        ("y", ((0, 1), (1, 0), (2, 3), (3, 2))),
        ("y", ((0, 2), (2, 0), (1, 3), (3, 1))),
    ):
        total = total + lax.ppermute(total, axis, pairs)
    return total


def stepped(grad, diag, first, second):
    first_new = beta_one * first + (1.0 - beta_one) * grad
    second_new = beta_two * second + (1.0 - beta_two) * diag * diag
    direction = (
        first_new
        / (1.0 - beta_one**STEP)
        / (jnp.sqrt(second_new / (1.0 - beta_two**STEP)) + adam_eps)
    )
    return (first_new, second_new, direction)


def local(
    tokens,
    targets,
    norm_gain,
    up_master,
    down_master,
    up_probe,
    down_probe,
    up_first,
    up_second,
    down_first,
    down_second,
):
    rows, width = tokens.shape
    own_rows, hidden = up_master.shape
    tokens_all = jnp.float32(rows * lax.axis_size(DP))
    index = lax.axis_index(DP)
    z = lax.axis_index("z")

    up_full = gathered(up_master.astype(jnp.bfloat16), DP)
    down_own = after(down_master.T.astype(jnp.bfloat16), up_full[:16, :128])
    down_full = gathered(down_own, DP)
    up_signs = signs_rows(up_probe)
    down_probe_t = down_probe.T
    down_signs = signs_rows(down_probe_t)

    values = tokens.astype(jnp.float32)
    scale = lax.rsqrt(jnp.mean(values * values, axis=-1, keepdims=True) + norm_eps)
    normed = (values * scale * norm_gain).astype(jnp.bfloat16)
    preact_dir = dot_plain(normed, up_signs)
    preact = dot_plain(normed, up_full)
    logistic = jax.nn.sigmoid(preact)
    active = (preact * logistic).astype(jnp.bfloat16)
    slopes = logistic * (1.0 + preact * (1.0 - logistic))
    curves = logistic * (1.0 - logistic) * (2.0 + preact * (1.0 - 2.0 * logistic))
    active_dir = (slopes * preact_dir).astype(jnp.bfloat16)

    acts = interleaved(active_dir, active)
    lead = interleaved(active, active_dir)
    side = interleaved(jnp.zeros_like(active), active)
    partial = dot_last(lead, down_full) + dot_last(side, down_signs)
    partial = partial.astype(jnp.bfloat16)
    scattered = lax.psum_scatter(partial, "z", scatter_dimension=0, tiled=True)

    acts_later, normed_later = lax.optimization_barrier((acts, normed, partial))[:2]
    acts_all = sent_to_all(acts_later, DP).reshape(-1, hidden)
    inputs = lax.all_to_all(normed_later, DP, split_axis=1, concat_axis=0, tiled=True)

    other = lax.ppermute(scattered, "xhi", ((0, 1), (1, 0)))
    total = scattered.astype(jnp.float32) + other.astype(jnp.float32)
    few = rows // N_Z
    goal = lax.dynamic_slice_in_dim(targets, z * few, few, 0).astype(jnp.float32)
    less = jnp.concatenate([goal, jnp.zeros_like(goal)], axis=0)
    own_res = ((total - less) / tokens_all).astype(jnp.bfloat16)
    res_both = gathered(own_res, "z")

    res_all = lax.all_to_all(res_both, DP, split_axis=1, concat_axis=0, tiled=True)
    residual, _ = apart(res_both)
    res32 = residual.astype(jnp.float32)
    loss = over_pairs(0.5 * jnp.sum(res32 * res32) * tokens_all)

    main = dot_plain(res_both, down_full)
    extra = dot_plain(res_both, down_signs)
    grad_active, hess_active = apart(main)
    hess_active = hess_active + apart(extra)[0]
    grad_preact = (slopes * grad_active).astype(jnp.bfloat16)
    hess_preact = (curves * preact_dir * grad_active + slopes * hess_active).astype(jnp.bfloat16)
    grads_all = gathered(jnp.stack([grad_preact, hess_preact])[None], DP)

    down_hess = dot_first(res_all, acts_all)
    blocks = acts_all.shape[0] // (2 * few)
    act_all = acts_all.reshape(blocks, 2, few, hidden)[:, 1].reshape(-1, hidden)
    resid_all = res_all.reshape(blocks, 2, few, own_rows)[:, 0].reshape(-1, own_rows)
    down_grad = dot_first(resid_all, act_all)
    up_grad = dot_first(inputs, grads_all[:, 0].reshape(-1, hidden))
    up_hess = dot_first(inputs, grads_all[:, 1].reshape(-1, hidden))

    up_hut = jnp.abs(own_signs(up_probe, index) * up_hess)
    spot = lax.broadcasted_iota(jnp.int32, (hidden, hidden), 0) // BLOCK
    place = lax.broadcasted_iota(jnp.int32, (hidden, hidden), 1) // BLOCK
    average = jnp.where(spot == place, 1.0 / BLOCK, 0.0).astype(jnp.float32)
    up_diag = jnp.dot(up_hut, average, precision=lax.Precision.HIGHEST)
    down_hut = jnp.abs(own_signs(down_probe_t, index) * down_hess)
    means = jnp.mean(down_hut.reshape(own_rows // BLOCK, BLOCK, hidden), axis=1)
    down_diag = jnp.repeat(means, BLOCK, axis=0)
    up_out = stepped(up_grad, up_diag, up_first, up_second)
    down_out = stepped(down_grad, down_diag, down_first.T, down_second.T)
    return (loss, *up_out, *(v.T for v in down_out))


def solution(mesh):
    fine = Mesh(mesh.devices.reshape(4, 2, 2, N_Z, 2), (*DP, *FS))
    placed = (
        P(DP, None),
        P(DP, None),
        P(),
        P(DP, FS),
        P(FS, DP),
        P(None, FS),
        P(FS, None),
        P(DP, FS),
        P(DP, FS),
        P(FS, DP),
        P(FS, DP),
    )
    return jax.shard_map(
        local,
        mesh=fine,
        in_specs=placed,
        out_specs=(P(), P(DP, FS), P(DP, FS), P(DP, FS), P(FS, DP), P(FS, DP), P(FS, DP)),
        check_vma=False,
    )
```

```python
import jax
import jax.numpy as jnp
from jax import lax
from jax.experimental import pallas as pl
from jax.experimental.pallas import tpu as pltpu
from jax.sharding import Mesh, PartitionSpec as P


BLOCK = 16
STEP = 10
N_Z = 8
N_Y = 4
N_DP = 16

norm_eps = 1e-05
beta_one = 0.9
beta_two = 0.999
adam_eps = 1e-08

DP = ("y", "xlo", "core")
FS = ("z", "xhi")


def dot_first(left, right):
    return lax.dot_general(
        left, right, (((0,), (0,)), ((), ())), preferred_element_type=jnp.float32
    )


def dot_plain(left, right):
    return jnp.dot(left, right, preferred_element_type=jnp.float32)


def signs_of(probe, blocks):
    shifts = (2 * blocks[:, None] + jnp.arange(2, dtype=jnp.int32)[None]).reshape(-1, 1, 1)
    bits = jnp.bitwise_and(jnp.right_shift(probe[None, :, :], shifts), 1)
    return (1 - 2 * bits).reshape(-1, probe.shape[1]).astype(jnp.bfloat16)


def after(value, *others):
    return lax.optimization_barrier((value, *others))[0]


def from_along(value, axis, step):
    size = lax.axis_size(axis)
    return lax.ppermute(value, axis, [(s, (s - step) % size) for s in range(size)])


def gather_dp(shard, place):
    y, x, c = (lax.axis_index(a) for a in DP)
    rows = shard.shape[0]
    half = rows // 2
    below = from_along(shard, "y", -1)
    above = from_along(shard, "y", 1)
    beside = from_along(shard, "xlo", 1)
    far_one = from_along(below[:half], "y", -1)
    far_two = from_along(above[half:], "y", 1)
    beside_above = from_along(above, "xlo", 1)
    beside_below = from_along(beside, "y", -1)
    beside_far = from_along(beside_above, "y", 1)
    pieces = (
        (shard, 0, 0, 0),
        (below, -1, 0, 0),
        (above, 1, 0, 0),
        (beside, 0, 1, 0),
        (far_one, 2, 0, 0),
        (far_two, 2, 0, half),
        (beside_above, 1, 1, 0),
        (beside_below, -1, 1, 0),
        (beside_far, 2, 1, 0),
    )
    full = jnp.zeros((N_DP, *shard.shape), shard.dtype)
    for swap in (0, 1):
        for piece, dy, dx, start in pieces:
            got = from_along(piece, "core", 1) if swap else piece
            source = (((y + dy) % N_Y) * 2 + (x + dx) % 2) * 2 + (c + swap) % 2
            full = lax.dynamic_update_slice(full, got[None], (place(source), start, 0))
    return full


def over_pairs(value):
    total = value
    for axis, pairs in (
        ("core", ((0, 1), (1, 0))),
        ("xlo", ((0, 1), (1, 0))),
        ("y", ((0, 1), (1, 0), (2, 3), (3, 2))),
        ("y", ((0, 2), (2, 0), (1, 3), (3, 1))),
    ):
        total = total + lax.ppermute(total, axis, pairs)
    return total


def last_last(left, right):
    return lax.dot_general(
        left, right, (((1,), (1,)), ((), ())), preferred_element_type=jnp.float32
    )


def down_kernel(res_ref, act_ref, grad_ref, hess_ref):
    @pl.when(pl.program_id(0) == 0)
    def _():
        grad_ref[...] = jnp.zeros_like(grad_ref)
        hess_ref[...] = jnp.zeros_like(hess_ref)

    res = res_ref[0]
    act = act_ref[0]
    tok = res.shape[1] // 2
    grad_ref[...] += last_last(res[:, :tok], act[:, tok:])
    hess_ref[...] += last_last(res, act)


def up_kernel(in_ref, out_ref, grad_ref, hess_ref):
    @pl.when(pl.program_id(0) == 0)
    def _():
        grad_ref[...] = jnp.zeros_like(grad_ref)
        hess_ref[...] = jnp.zeros_like(hess_ref)

    normed = in_ref[0]
    back = out_ref[0]
    tok = normed.shape[1]
    grad_ref[...] += last_last(normed, back[:, :tok])
    hess_ref[...] += last_last(normed, back[:, tok:])


def weight_products(kernel, name, left, right):
    count, rows, cols = left.shape
    hidden = right.shape[1]
    shape = jax.ShapeDtypeStruct((rows, hidden), jnp.float32)
    return pl.pallas_call(
        kernel,
        grid=(count,),
        in_specs=[
            pl.BlockSpec((1, rows, cols), lambda b: (b, 0, 0)),
            pl.BlockSpec((1, hidden, right.shape[2]), lambda b: (b, 0, 0)),
        ],
        out_specs=[pl.BlockSpec((rows, hidden), lambda b: (0, 0))] * 2,
        out_shape=[shape, shape],
        name=name,
        cost_estimate=pl.CostEstimate(
            flops=4 * count * rows * hidden * 128, bytes_accessed=10_000_000, transcendentals=0
        ),
    )(left, right)


def stepped(grad, diag, first, second):
    first_new = beta_one * first + (1.0 - beta_one) * grad
    second_new = beta_two * second + (1.0 - beta_two) * diag * diag
    direction = (
        first_new
        / (1.0 - beta_one**STEP)
        / (jnp.sqrt(second_new / (1.0 - beta_two**STEP)) + adam_eps)
    )
    return (first_new, second_new, direction)


def local(
    tokens,
    targets,
    norm_gain,
    up_master,
    down_master,
    up_probe,
    down_probe,
    up_first,
    up_second,
    down_first,
    down_second,
):
    rows, width = tokens.shape
    own_rows, hidden = up_master.shape
    tokens_all = jnp.float32(rows * lax.axis_size(DP))
    index = lax.axis_index(DP)
    z = lax.axis_index("z")
    order = (index + jnp.arange(N_DP, dtype=jnp.int32)) % N_DP

    packed = jnp.concatenate(
        [up_master.astype(jnp.bfloat16), down_master.T.astype(jnp.bfloat16)], axis=1
    )
    weights = gather_dp(packed, lambda s: (s - index) % N_DP).reshape(width, 2 * hidden)
    up_full = weights[:, :hidden]
    down_full = weights[:, hidden:]
    down_probe_t = down_probe.T
    up_signs = signs_of(up_probe, order)
    down_signs = signs_of(down_probe_t, order)

    values = tokens.T.astype(jnp.float32)
    scale = lax.rsqrt(jnp.mean(values * values, axis=0, keepdims=True) + norm_eps)
    normed = (values * scale * norm_gain[:, None]).astype(jnp.bfloat16)
    normed = normed.reshape(N_DP, own_rows, rows)
    twice = jnp.concatenate([normed, normed], axis=0)
    rolled = lax.dynamic_slice_in_dim(twice, index, N_DP, 0).reshape(width, rows)
    few = width // N_Z
    goal = jnp.concatenate(
        [
            lax.dynamic_slice_in_dim(targets, order_at * own_rows, own_rows, 1).T
            for order_at in ((index + 2 * z) % N_DP, (index + 2 * z + 1) % N_DP)
        ],
        axis=0,
    ).astype(jnp.float32)

    preact_dir = dot_first(up_signs, rolled)
    preact = dot_first(up_full, rolled)
    logistic = jax.nn.sigmoid(preact)
    active = (preact * logistic).astype(jnp.bfloat16)
    slopes = logistic * (1.0 + preact * (1.0 - logistic))
    curves = logistic * (1.0 - logistic) * (2.0 + preact * (1.0 - 2.0 * logistic))
    active_dir = (slopes * preact_dir).astype(jnp.bfloat16)

    lead = jnp.concatenate([active, active_dir], axis=1)
    side = jnp.concatenate([jnp.zeros_like(active), active], axis=1)
    partial = (dot_plain(down_full, lead) + dot_plain(down_signs, side)).astype(jnp.bfloat16)
    scattered = lax.psum_scatter(partial, "z", scatter_dimension=0, tiled=True)

    acts = after(jnp.concatenate([active_dir, active], axis=1), partial)
    acts_all = gather_dp(acts, lambda s: (index - s) % N_DP)
    scattered = after(scattered, acts_all)

    other = lax.ppermute(scattered, "xhi", ((0, 1), (1, 0)))
    total = scattered.astype(jnp.float32) + other.astype(jnp.float32)
    less = jnp.concatenate([goal, jnp.zeros_like(goal)], axis=1)
    own_res = ((total - less) / tokens_all).astype(jnp.bfloat16)
    res_both = lax.all_gather(own_res, "z", axis=0, tiled=True)

    moved = []
    for k in (0, 1):
        pairs = [
            (i * N_Z + zz, ((i + 2 * zz + k) % N_DP) * N_Z + zz)
            for i in range(N_DP)
            for zz in range(N_Z)
        ]
        piece = own_res[k * own_rows : (k + 1) * own_rows]
        moved.append(lax.ppermute(piece, (*DP, "z"), pairs))
    inputs = lax.all_to_all(after(normed, own_res), DP, 0, 0, tiled=True)
    res_both, inputs, *moved = lax.optimization_barrier((res_both, inputs, *moved))
    res_all = lax.all_gather(jnp.stack(moved), "z", axis=0, tiled=True)

    main = dot_first(down_full, res_both)
    extra = dot_first(down_signs, res_both[:, :rows])
    grad_active = main[:, :rows]
    hess_active = main[:, rows:] + extra
    grad_preact = (slopes * grad_active).astype(jnp.bfloat16)
    hess_preact = (curves * preact_dir * grad_active + slopes * hess_active).astype(jnp.bfloat16)
    grads = jnp.concatenate([grad_preact, hess_preact], axis=1)
    grads_all = gather_dp(grads, lambda s: s)

    res32 = after(res_both, grads)[:, :rows].astype(jnp.float32)
    loss = over_pairs(0.5 * jnp.sum(res32 * res32) * tokens_all)

    up_grad, up_hess = weight_products(up_kernel, "up_products", inputs, grads_all)
    down_grad, down_hess = weight_products(down_kernel, "down_products", res_all, acts_all)

    own = index[None]
    up_hut = jnp.abs(signs_of(up_probe, own).astype(jnp.float32) * up_hess)
    spot = lax.broadcasted_iota(jnp.int32, (hidden, hidden), 0) // BLOCK
    spread = lax.broadcasted_iota(jnp.int32, (hidden, hidden), 1) // BLOCK
    average = jnp.where(spot == spread, 1.0 / BLOCK, 0.0).astype(jnp.float32)
    up_diag = jnp.dot(up_hut, average, precision=lax.Precision.HIGHEST)
    down_hut = jnp.abs(signs_of(down_probe_t, own).astype(jnp.float32) * down_hess)
    means = jnp.mean(down_hut.reshape(own_rows // BLOCK, BLOCK, hidden), axis=1)
    down_diag = jnp.repeat(means, BLOCK, axis=0)
    up_out = stepped(up_grad, up_diag, up_first, up_second)
    down_out = stepped(down_grad, down_diag, down_first.T, down_second.T)
    return (loss, *up_out, *(v.T for v in down_out))


def solution(mesh):
    fine = Mesh(mesh.devices.reshape(N_Y, 2, 2, N_Z, 2), (*DP, *FS))
    placed = (
        P(DP, None),
        P(DP, None),
        P(),
        P(DP, FS),
        P(FS, DP),
        P(None, FS),
        P(FS, None),
        P(DP, FS),
        P(DP, FS),
        P(FS, DP),
        P(FS, DP),
    )
    return jax.shard_map(
        local,
        mesh=fine,
        in_specs=placed,
        out_specs=(P(), P(DP, FS), P(DP, FS), P(DP, FS), P(FS, DP), P(FS, DP), P(FS, DP)),
        check_vma=False,
    )
```

```python
import jax
import jax.numpy as jnp
from jax import lax
from jax.experimental import pallas as pl
from jax.experimental.pallas import tpu as pltpu
from jax.sharding import Mesh, PartitionSpec as P


BLOCK = 16
STEP = 10
N_Z = 8
N_Y = 4
N_DP = 16

norm_eps = 1e-05
beta_one = 0.9
beta_two = 0.999
adam_eps = 1e-08

DP = ("y", "xlo", "core")
FS = ("z", "xhi")
LANES = 128
MAIN = 384


def dot_first(left, right):
    return lax.dot_general(
        left, right, (((0,), (0,)), ((), ())), preferred_element_type=jnp.float32
    )


def dot_plain(left, right):
    return jnp.dot(left, right, preferred_element_type=jnp.float32)


def signs_of(probe, blocks):
    shifts = (2 * blocks[:, None] + jnp.arange(2, dtype=jnp.int32)[None]).reshape(-1, 1, 1)
    bits = jnp.bitwise_and(jnp.right_shift(probe[None, :, :], shifts), 1)
    return (1 - 2 * bits).reshape(-1, probe.shape[1]).astype(jnp.bfloat16)


def after(value, *others):
    return lax.optimization_barrier((value, *others))[0]


def from_along(value, axis, step):
    size = lax.axis_size(axis)
    return lax.ppermute(value, axis, [(s, (s - step) % size) for s in range(size)])


def gather_chips(shard):
    half = shard.shape[0] // 2
    below = from_along(shard, "y", -1)
    above = from_along(shard, "y", 1)
    beside = from_along(shard, "xlo", 1)
    far = (from_along(below[:half], "y", -1), from_along(above[half:], "y", 1))
    beside_above = from_along(above, "xlo", 1)
    beside_below = from_along(beside, "y", -1)
    beside_far = from_along(beside_above, "y", 1)
    return {
        (0, 0): (shard,),
        (0, 1): (beside,),
        (1, 0): (above,),
        (1, 1): (beside_above,),
        (2, 0): far,
        (2, 1): (beside_far,),
        (3, 0): (below,),
        (3, 1): (beside_below,),
    }


def gather_dp(shard):
    pieces = gather_chips(shard)
    full = {}
    for step, parts in pieces.items():
        full[(*step, 0)] = parts
        full[(*step, 1)] = tuple(from_along(p, "core", 1) for p in parts)
    return full


STEPS = [(dy, dx, dc) for dy in range(N_Y) for dx in range(2) for dc in range(2)]


def flat(pieces):
    return [p for step in sorted(pieces) for p in pieces[step]]


def read_all(refs, steps, far):
    refs = list(refs)
    out = {}
    for step in steps:
        if far(step):
            out[step] = jnp.concatenate([refs.pop(0)[...], refs.pop(0)[...]], axis=0)
        else:
            out[step] = refs.pop(0)[...]
    return out


def is_far(step):
    return step[:2] == (2, 0)


def over_pairs(value):
    total = value
    for axis, pairs in (
        ("core", ((0, 1), (1, 0))),
        ("xlo", ((0, 1), (1, 0))),
        ("y", ((0, 1), (1, 0), (2, 3), (3, 2))),
        ("y", ((0, 2), (2, 0), (1, 3), (3, 1))),
    ):
        total = total + lax.ppermute(total, axis, pairs)
    return total


def last_last(left, right):
    return lax.dot_general(
        left, right, (((1,), (1,)), ((), ())), preferred_element_type=jnp.float32
    )


def block_signs(words, block):
    halves = [1 - 2 * ((words >> (2 * block + h)) & 1) for h in (0, 1)]
    return jnp.concatenate(halves, axis=0).astype(jnp.float32).astype(jnp.bfloat16)


def dir_kernel(probe_ref, normed_ref, out_ref):
    words = probe_ref[...]
    out_ref[...] = jnp.zeros_like(out_ref)

    def step(r, carry):
        out_ref[...] += dot_plain(normed_ref[r], block_signs(words, r))
        return carry

    lax.fori_loop(0, N_DP, step, 0)


def forward_kernel(order_ref, probe_ref, normed_ref, dir_ref, *refs):
    piece_refs, (part_ref, acts_ref, slopes_ref, cross_ref) = refs[:-4], refs[-4:]
    weights = read_all(piece_refs, STEPS, is_far)
    rows = normed_ref.shape[1]
    hidden = dir_ref.shape[1]
    main = jnp.zeros((rows, MAIN), jnp.float32)
    tail = jnp.zeros((rows, LANES), jnp.float32)
    for r, step in enumerate(STEPS):
        normed = normed_ref[order_ref[r]]
        main += dot_plain(normed, weights[step][:, :MAIN])
        tail += dot_plain(normed, weights[step][:, 2 * MAIN :])
    rest = hidden - MAIN
    preact = jnp.concatenate([main, tail[:, :rest]], axis=1)
    preact_dir = dir_ref[...]
    logistic = jax.nn.sigmoid(preact)
    active = (preact * logistic).astype(jnp.bfloat16)
    slopes = logistic * (1.0 + preact * (1.0 - logistic))
    curves = logistic * (1.0 - logistic) * (2.0 + preact * (1.0 - 2.0 * logistic))
    active_dir = (slopes * preact_dir).astype(jnp.bfloat16)
    slopes_ref[...] = slopes
    cross_ref[...] = curves * preact_dir
    acts_ref[:rows] = active_dir
    acts_ref[rows:] = active
    lead = jnp.concatenate([active, active_dir], axis=0)
    ends = jnp.concatenate(
        [
            jnp.zeros((2 * rows, rest), jnp.bfloat16),
            lead[:, MAIN:],
            jnp.zeros((2 * rows, LANES - 2 * rest), jnp.bfloat16),
        ],
        axis=1,
    )
    words = probe_ref[...]
    own = 2 * words.shape[0]
    for r, step in enumerate(STEPS):
        out = last_last(weights[step][:, MAIN : 2 * MAIN], lead[:, :MAIN])
        out += last_last(weights[step][:, 2 * MAIN :], ends)
        side = last_last(block_signs(words, order_ref[r]), active)
        at = slice(r * own, (r + 1) * own)
        part_ref[at, :rows] = out[:, :rows].astype(jnp.bfloat16)
        part_ref[at, rows:] = (out[:, rows:] + side).astype(jnp.bfloat16)


def backward_kernel(order_ref, probe_ref, res_ref, slopes_ref, cross_ref, *refs):
    piece_refs, out_ref = refs[:-1], refs[-1]
    weights = read_all(piece_refs, STEPS, is_far)
    words = probe_ref[...]
    own = 2 * words.shape[0]
    rows, hidden = slopes_ref.shape
    main = jnp.zeros((2 * rows, MAIN), jnp.float32)
    tail = jnp.zeros((2 * rows, LANES), jnp.float32)
    side = jnp.zeros((rows, hidden), jnp.float32)
    for r, step in enumerate(STEPS):
        res = res_ref[r * own : (r + 1) * own, :]
        main += dot_first(res, weights[step][:, MAIN : 2 * MAIN])
        tail += dot_first(res, weights[step][:, 2 * MAIN :])
        side += dot_first(res[:, :rows], block_signs(words, order_ref[r]))
    rest = hidden - MAIN
    both = jnp.concatenate([main, tail[:, rest : 2 * rest]], axis=1)
    grad_active = both[:rows]
    hess_active = both[rows:] + side
    slopes = slopes_ref[...]
    out_ref[:rows] = (slopes * grad_active).astype(jnp.bfloat16)
    out_ref[rows:] = (cross_ref[...] * grad_active + slopes * hess_active).astype(jnp.bfloat16)


def down_kernel(res_ref, *refs):
    piece_refs, (grad_ref, hess_ref) = refs[:-2], refs[-2:]
    chips = sorted({step[:2] for step in STEPS})
    acts = read_all(piece_refs, chips, is_far)
    own = [((N_Y - dy) % N_Y * 2 + dx) * 2 + dc for dy, dx, dc in STEPS]
    tok = res_ref.shape[2] // 2
    left = jnp.concatenate([res_ref[r] for r in own], axis=1)
    right = jnp.concatenate([acts[chip] for chip in chips], axis=0)
    hess_ref[...] = dot_plain(left, right)
    left = jnp.concatenate([res_ref[r, :, :tok] for r in own], axis=1)
    rows = [2 * tok * q for q in (0, 1)]
    right = jnp.concatenate(
        [acts[chip][q + tok : q + 2 * tok] for chip in chips for q in rows], axis=0
    )
    grad_ref[...] = dot_plain(left, right)


def up_kernel(order_ref, in_ref, *refs):
    piece_refs, (grad_ref, hess_ref) = refs[:-2], refs[-2:]
    grads = read_all(piece_refs, STEPS, is_far)
    tok = in_ref.shape[2]
    left = jnp.concatenate([in_ref[order_ref[r]] for r in range(N_DP)], axis=1)
    grad_ref[...] = dot_plain(left, jnp.concatenate([grads[s][:tok] for s in STEPS], axis=0))
    hess_ref[...] = dot_plain(left, jnp.concatenate([grads[s][tok:] for s in STEPS], axis=0))


def call(kernel, name, outs, flops, *operands):
    in_specs = [
        pl.BlockSpec(memory_space=pltpu.SMEM if o.ndim == 1 else pltpu.VMEM) for o in operands
    ]
    return pl.pallas_call(
        kernel,
        in_specs=in_specs,
        out_specs=jax.tree.map(lambda _: pl.BlockSpec(memory_space=pltpu.VMEM), outs),
        out_shape=outs,
        name=name,
        cost_estimate=pl.CostEstimate(
            flops=flops,
            bytes_accessed=sum(o.size * o.dtype.itemsize for o in operands),
            transcendentals=0,
        ),
    )(*operands)


def stepped(grad, diag, first, second):
    first_new = beta_one * first + (1.0 - beta_one) * grad
    second_new = beta_two * second + (1.0 - beta_two) * diag * diag
    direction = (
        first_new
        / (1.0 - beta_one**STEP)
        / (jnp.sqrt(second_new / (1.0 - beta_two**STEP)) + adam_eps)
    )
    return (first_new, second_new, direction)


def local(
    tokens,
    targets,
    norm_gain,
    up_master,
    down_master,
    up_probe,
    down_probe,
    up_first,
    up_second,
    down_first,
    down_second,
):
    rows, width = tokens.shape
    own_rows, hidden = up_master.shape
    tokens_all = jnp.float32(rows * lax.axis_size(DP))
    index = lax.axis_index(DP)
    z = lax.axis_index("z")
    y, x, c = (lax.axis_index(a) for a in DP)
    place = lambda dy, dx, dc: (((y + dy) % N_Y) * 2 + (x + dx) % 2) * 2 + (c + dc) % 2
    order = jnp.stack([place(*step) for step in STEPS]).astype(jnp.int32)

    up_cast = up_master.astype(jnp.bfloat16)
    down_cast = down_master.T.astype(jnp.bfloat16)
    spare = jnp.zeros((own_rows, LANES - 2 * (hidden - MAIN)), jnp.bfloat16)
    packed = jnp.concatenate(
        [up_cast[:, :MAIN], down_cast[:, :MAIN], up_cast[:, MAIN:], down_cast[:, MAIN:], spare],
        axis=1,
    )
    weights = flat(gather_dp(packed))
    down_probe_t = down_probe.T

    values = tokens.astype(jnp.float32)
    scale = lax.rsqrt(jnp.mean(values * values, axis=1, keepdims=True) + norm_eps)
    normed = (values * scale * norm_gain).astype(jnp.bfloat16)
    normed = jnp.stack(
        [normed[:, r * own_rows : (r + 1) * own_rows] for r in range(N_DP)]
    )
    few = width // N_Z
    goal = jnp.concatenate(
        [
            lax.dynamic_slice_in_dim(
                targets, place(z // 2, z % 2, k) * own_rows, own_rows, 1
            ).T
            for k in (0, 1)
        ],
        axis=0,
    ).astype(jnp.float32)

    thin = jax.ShapeDtypeStruct((rows, hidden), jnp.float32)
    pair = jax.ShapeDtypeStruct((2 * rows, hidden), jnp.bfloat16)
    step_flops = 2 * rows * width * hidden
    preact_dir = call(dir_kernel, "dir", thin, step_flops, up_probe, normed)
    partial, acts, slopes, cross = call(
        forward_kernel,
        "forward",
        [jax.ShapeDtypeStruct((width, 2 * rows), jnp.bfloat16), pair, thin, thin],
        4 * step_flops,
        order,
        down_probe_t,
        normed,
        preact_dir,
        *weights,
    )
    scattered = lax.psum_scatter(partial, "z", scatter_dimension=0, tiled=True)

    acts_pair = jnp.concatenate([acts, from_along(acts, "core", 1)], axis=0)
    acts_all = flat(gather_chips(acts_pair))
    scattered, *acts_all = lax.optimization_barrier((scattered, *acts_all))

    other = lax.ppermute(scattered, "xhi", ((0, 1), (1, 0)))
    total = scattered.astype(jnp.float32) + other.astype(jnp.float32)
    less = jnp.concatenate([goal, jnp.zeros_like(goal)], axis=1)
    own_res = ((total - less) / tokens_all).astype(jnp.bfloat16)
    res_both = lax.all_gather(own_res, "z", axis=0, tiled=True)

    moved = []
    for k in (0, 1):
        pairs = [
            (
                (((yy * 2 + xx) * 2) + cc) * N_Z + zz,
                ((((yy + zz // 2) % N_Y * 2) + (xx + zz) % 2) * 2 + (cc + k) % 2) * N_Z + zz,
            )
            for yy in range(N_Y)
            for xx in range(2)
            for cc in range(2)
            for zz in range(N_Z)
        ]
        piece = own_res[k * own_rows : (k + 1) * own_rows]
        moved.append(lax.ppermute(piece, (*DP, "z"), pairs))
    normed_t = after(normed, own_res).swapaxes(1, 2)
    inputs = lax.all_to_all(normed_t, DP, 0, 0, tiled=True)
    moved_both = jnp.stack(moved)
    res_both, inputs, moved_both = lax.optimization_barrier((res_both, inputs, moved_both))
    res_all = lax.all_gather(moved_both, "z", axis=0, tiled=True)

    grads = call(
        backward_kernel,
        "backward",
        pair,
        3 * step_flops,
        order,
        down_probe_t,
        res_both,
        slopes,
        cross,
        *weights,
    )
    grads_all = flat(gather_dp(grads))
    res_late, *grads_all = lax.optimization_barrier((res_both, *grads_all))
    res32 = res_late[:, :rows].astype(jnp.float32)
    loss = over_pairs(0.5 * jnp.sum(res32 * res32) * tokens_all)

    wide = jax.ShapeDtypeStruct((own_rows, hidden), jnp.float32)
    up_grad, up_hess = call(
        up_kernel, "up_products", [wide, wide], 2 * step_flops, order, inputs, *grads_all
    )
    down_grad, down_hess = call(
        down_kernel, "down_products", [wide, wide], 3 * step_flops, res_all, *acts_all
    )

    own = index[None]
    up_hut = jnp.abs(signs_of(up_probe, own).astype(jnp.float32) * up_hess)
    spot = lax.broadcasted_iota(jnp.int32, (hidden, hidden), 0) // BLOCK
    spread = lax.broadcasted_iota(jnp.int32, (hidden, hidden), 1) // BLOCK
    average = jnp.where(spot == spread, 1.0 / BLOCK, 0.0).astype(jnp.float32)
    up_diag = jnp.dot(up_hut, average, precision=lax.Precision.HIGHEST)
    down_hut = jnp.abs(signs_of(down_probe_t, own).astype(jnp.float32) * down_hess)
    means = jnp.mean(down_hut.reshape(own_rows // BLOCK, BLOCK, hidden), axis=1)
    down_diag = jnp.repeat(means, BLOCK, axis=0)
    up_out = stepped(up_grad, up_diag, up_first, up_second)
    down_out = stepped(down_grad, down_diag, down_first.T, down_second.T)
    return (loss, *up_out, *(v.T for v in down_out))


def solution(mesh):
    fine = Mesh(mesh.devices.reshape(N_Y, 2, 2, N_Z, 2), (*DP, *FS))
    placed = (
        P(DP, None),
        P(DP, None),
        P(),
        P(DP, FS),
        P(FS, DP),
        P(None, FS),
        P(FS, None),
        P(DP, FS),
        P(DP, FS),
        P(FS, DP),
        P(FS, DP),
    )
    return jax.shard_map(
        local,
        mesh=fine,
        in_specs=placed,
        out_specs=(P(), P(DP, FS), P(DP, FS), P(DP, FS), P(FS, DP), P(FS, DP), P(FS, DP)),
        check_vma=False,
    )
```

```python
import jax
import jax.numpy as jnp
from jax import lax
from jax.experimental import pallas as pl
from jax.experimental.pallas import tpu as pltpu
from jax.sharding import Mesh, PartitionSpec as P


BLOCK = 16
STEP = 10
N_Z = 8
N_Y = 4
N_DP = 16

norm_eps = 1e-05
beta_one = 0.9
beta_two = 0.999
adam_eps = 1e-08

DP = ("y", "xlo", "core")
FS = ("z", "xhi")
LANES = 128
MAIN = 384
EXTRA = 32


def dot_first(left, right):
    return lax.dot_general(
        left, right, (((0,), (0,)), ((), ())), preferred_element_type=jnp.float32
    )


def dot_plain(left, right):
    return jnp.dot(left, right, preferred_element_type=jnp.float32)


def signs_of(probe, blocks):
    shifts = (2 * blocks[:, None] + jnp.arange(2, dtype=jnp.int32)[None]).reshape(-1, 1, 1)
    bits = jnp.bitwise_and(jnp.right_shift(probe[None, :, :], shifts), 1)
    return (1 - 2 * bits).reshape(-1, probe.shape[1]).astype(jnp.bfloat16)


def after(value, *others):
    return lax.optimization_barrier((value, *others))[0]


def from_along(value, axis, step):
    size = lax.axis_size(axis)
    return lax.ppermute(value, axis, [(s, (s - step) % size) for s in range(size)])


def fenced(values):
    return list(lax.optimization_barrier(tuple(values)))


def gather_chips(shard, swap, split, also=()):
    half = shard.shape[0] // 2
    parts = {(0, 0): [shard]}
    others = {}

    def cross(*steps):
        if swap:
            for step in steps:
                others[step] = [from_along(p, "core", 1) for p in parts[step]]

    def arrive(steps, extra=()):
        held = [(table, step) for step in steps for table in (parts, others) if step in table]
        lens = [len(table[step]) for table, step in held]
        values = fenced([p for table, step in held for p in table[step]] + list(extra))
        for (table, step), n in zip(held, lens):
            table[step], values = values[:n], values[n:]
        return values

    cross((0, 0))
    parts[3, 0] = [from_along(shard, "y", -1)]
    parts[1, 0] = [from_along(shard, "y", 1)]
    parts[0, 1] = [from_along(shard, "xlo", 1)]
    arrive([(3, 0), (1, 0), (0, 1)])
    cross((3, 0), (1, 0), (0, 1))
    parts[2, 0] = [from_along(parts[1, 0][0], "y", 1)]
    parts[3, 1] = [from_along(parts[0, 1][0], "y", -1)]
    parts[1, 1] = [from_along(parts[1, 0][0], "xlo", 1)]
    also = arrive([(2, 0), (3, 1), (1, 1), (3, 0), (1, 0), (0, 1)], also)
    if split:
        parts[2, 1] = [
            from_along(parts[2, 0][0][:half], "xlo", 1),
            from_along(parts[1, 1][0][half:], "y", 1),
        ]
    else:
        parts[2, 1] = [from_along(parts[2, 0][0], "xlo", 1)]
    cross((2, 0), (3, 1), (1, 1))
    arrive([(2, 1)])
    cross((2, 1))
    if swap:
        parts = {(*k, dc): t[k] for dc, t in enumerate((parts, others)) for k in t}
    return [p for step in sorted(parts) for p in parts[step]], also


STEPS = [(dy, dx, dc) for dy in range(N_Y) for dx in range(2) for dc in range(2)]


def read_all(refs, steps, split=False):
    refs = list(refs)
    out = {}
    for step in steps:
        if split and step[:2] == (2, 1):
            out[step] = jnp.concatenate([refs.pop(0)[...], refs.pop(0)[...]], axis=0)
        else:
            out[step] = refs.pop(0)[...]
    return out


def last_last(left, right):
    return lax.dot_general(
        left, right, (((1,), (1,)), ((), ())), preferred_element_type=jnp.float32
    )


def block_signs(words, block):
    halves = [1 - 2 * ((words >> (2 * block + h)) & 1) for h in (0, 1)]
    return jnp.concatenate(halves, axis=0).astype(jnp.float32).astype(jnp.bfloat16)


def dir_kernel(tokens_ref, gain_ref, probe_ref, normed_ref, out_ref):
    values = tokens_ref[...].astype(jnp.float32)
    scale = lax.rsqrt(jnp.mean(values * values, axis=1, keepdims=True) + norm_eps)
    normed = values * scale * gain_ref[...]
    own = normed_ref.shape[2]
    for r in range(N_DP):
        normed_ref[r] = normed[:, r * own : (r + 1) * own].astype(jnp.bfloat16)
    words = probe_ref[...]
    out_ref[...] = jnp.zeros_like(out_ref)

    def step(r, carry):
        out_ref[...] += dot_plain(normed_ref[r], block_signs(words, r))
        return carry

    lax.fori_loop(0, N_DP, step, 0)


def forward_kernel(order_ref, probe_ref, normed_ref, dir_ref, *refs):
    piece_refs, (part_ref, acts_ref, slopes_ref, cross_ref) = refs[:-4], refs[-4:]
    weights = read_all(piece_refs, STEPS, True)
    rows = normed_ref.shape[1]
    hidden = dir_ref.shape[1]
    main = jnp.zeros((rows, MAIN), jnp.float32)
    tail = jnp.zeros((rows, LANES), jnp.float32)
    for r, step in enumerate(STEPS):
        normed = normed_ref[order_ref[r]]
        main += dot_plain(normed, weights[step][:, :MAIN])
        tail += dot_plain(normed, weights[step][:, 2 * MAIN :])
    rest = hidden - MAIN
    preact = jnp.concatenate([main, tail[:, :rest]], axis=1)
    preact_dir = dir_ref[...]
    logistic = jax.nn.sigmoid(preact)
    active = (preact * logistic).astype(jnp.bfloat16)
    slopes = logistic * (1.0 + preact * (1.0 - logistic))
    curves = logistic * (1.0 - logistic) * (2.0 + preact * (1.0 - 2.0 * logistic))
    active_dir = (slopes * preact_dir).astype(jnp.bfloat16)
    slopes_ref[...] = slopes
    cross_ref[...] = curves * preact_dir
    acts_ref[:rows] = active_dir
    acts_ref[rows:] = active
    lead = jnp.concatenate([active, active_dir], axis=0)
    ends = jnp.concatenate(
        [
            jnp.zeros((2 * rows, rest), jnp.bfloat16),
            lead[:, MAIN:],
            jnp.zeros((2 * rows, LANES - 2 * rest), jnp.bfloat16),
        ],
        axis=1,
    )
    words = probe_ref[...]
    own = 2 * words.shape[0]
    for r, step in enumerate(STEPS):
        out = last_last(weights[step][:, MAIN : 2 * MAIN], lead[:, :MAIN])
        out += last_last(weights[step][:, 2 * MAIN :], ends)
        side = last_last(block_signs(words, order_ref[r]), active)
        at = slice(r * own, (r + 1) * own)
        part_ref[at, :rows] = out[:, :rows].astype(jnp.bfloat16)
        part_ref[at, rows:] = (out[:, rows:] + side).astype(jnp.bfloat16)


def backward_kernel(order_ref, probe_ref, res_ref, slopes_ref, cross_ref, *refs):
    piece_refs, out_ref = refs[:-1], refs[-1]
    weights = read_all(piece_refs, STEPS, True)
    words = probe_ref[...]
    own = 2 * words.shape[0]
    rows, hidden = slopes_ref.shape
    main = jnp.zeros((2 * rows, MAIN), jnp.float32)
    tail = jnp.zeros((2 * rows, LANES), jnp.float32)
    side = jnp.zeros((rows, hidden), jnp.float32)
    squares = jnp.zeros((1, rows), jnp.float32)
    for r, step in enumerate(STEPS):
        res = res_ref[r * own : (r + 1) * own, :]
        residual = res[:, :rows].astype(jnp.float32)
        squares += jnp.sum(residual * residual, axis=0, keepdims=True)
        main += dot_first(res, weights[step][:, MAIN : 2 * MAIN])
        tail += dot_first(res, weights[step][:, 2 * MAIN :])
        side += dot_first(res[:, :rows], block_signs(words, order_ref[r]))
    rest = hidden - MAIN
    both = jnp.concatenate([main, tail[:, rest : 2 * rest]], axis=1)
    grad_active = both[:rows]
    hess_active = both[rows:] + side
    slopes = slopes_ref[...]
    out_ref[:rows] = (slopes * grad_active).astype(jnp.bfloat16)
    hess = cross_ref[...] * grad_active + slopes * hess_active
    out_ref[rows : 2 * rows] = hess.astype(jnp.bfloat16)
    loss = jnp.sum(squares, axis=1, keepdims=True) * (0.5 * rows * N_DP)
    high = loss.astype(jnp.bfloat16).astype(jnp.float32)
    lane = lax.broadcasted_iota(jnp.int32, (EXTRA, hidden), 1)
    parts = jnp.where(lane == 0, high, jnp.where(lane == 1, loss - high, 0.0))
    out_ref[2 * rows :] = parts.astype(jnp.bfloat16)


def down_kernel(res_ref, *refs):
    piece_refs, (grad_ref, hess_ref) = refs[:-2], refs[-2:]
    chips = sorted({step[:2] for step in STEPS})
    acts = read_all(piece_refs, chips)
    own = [((N_Y - dy) % N_Y * 2 + dx) * 2 + dc for dy, dx, dc in STEPS]
    tok = res_ref.shape[2] // 2
    left = jnp.concatenate([res_ref[r] for r in own], axis=1)
    right = jnp.concatenate([acts[chip] for chip in chips], axis=0)
    hess_ref[...] = dot_plain(left, right)
    left = jnp.concatenate([res_ref[r, :, :tok] for r in own], axis=1)
    rows = [2 * tok * q for q in (0, 1)]
    right = jnp.concatenate(
        [acts[chip][q + tok : q + 2 * tok] for chip in chips for q in rows], axis=0
    )
    grad_ref[...] = dot_plain(left, right)


def up_kernel(order_ref, in_ref, *refs):
    piece_refs, (grad_ref, hess_ref, loss_ref, sums_ref) = refs[:-4], refs[-4:]
    grads = read_all(piece_refs, STEPS)
    tok = in_ref.shape[2]
    left = jnp.concatenate([in_ref[order_ref[r]] for r in range(N_DP)], axis=1)
    grad_ref[...] = dot_plain(left, jnp.concatenate([grads[s][:tok] for s in STEPS], axis=0))
    hess_ref[...] = dot_plain(
        left, jnp.concatenate([grads[s][tok : 2 * tok] for s in STEPS], axis=0)
    )
    for r, step in enumerate(STEPS):
        sums_ref[order_ref[r]] = grads[step][2 * tok : 2 * tok + 8, :LANES].astype(jnp.float32)
    total = sums_ref[0]
    for s in range(1, N_DP):
        total += sums_ref[s]
    loss_ref[...] = jnp.broadcast_to(total[:, 0:1] + total[:, 1:2], loss_ref.shape)


def call(kernel, name, outs, flops, *operands, scratch=()):
    in_specs = [
        pl.BlockSpec(memory_space=pltpu.SMEM if o.ndim == 1 else pltpu.VMEM) for o in operands
    ]
    return pl.pallas_call(
        kernel,
        in_specs=in_specs,
        out_specs=jax.tree.map(lambda _: pl.BlockSpec(memory_space=pltpu.VMEM), outs),
        out_shape=outs,
        scratch_shapes=scratch,
        name=name,
        cost_estimate=pl.CostEstimate(
            flops=flops,
            bytes_accessed=sum(o.size * o.dtype.itemsize for o in operands),
            transcendentals=0,
        ),
    )(*operands)


def stepped(grad, diag, first, second):
    first_new = beta_one * first + (1.0 - beta_one) * grad
    second_new = beta_two * second + (1.0 - beta_two) * diag * diag
    direction = (
        first_new
        / (1.0 - beta_one**STEP)
        / (jnp.sqrt(second_new / (1.0 - beta_two**STEP)) + adam_eps)
    )
    return (first_new, second_new, direction)


def local(
    tokens,
    targets,
    norm_gain,
    up_master,
    down_master,
    up_probe,
    down_probe,
    up_first,
    up_second,
    down_first,
    down_second,
):
    rows, width = tokens.shape
    own_rows, hidden = up_master.shape
    tokens_all = jnp.float32(rows * lax.axis_size(DP))
    index = lax.axis_index(DP)
    z = lax.axis_index("z")
    y, x, c = (lax.axis_index(a) for a in DP)
    place = lambda dy, dx, dc: (((y + dy) % N_Y) * 2 + (x + dx) % 2) * 2 + (c + dc) % 2
    order = jnp.stack([place(*step) for step in STEPS]).astype(jnp.int32)

    up_cast = up_master.astype(jnp.bfloat16)
    down_cast = down_master.T.astype(jnp.bfloat16)
    spare = jnp.zeros((own_rows, LANES - 2 * (hidden - MAIN)), jnp.bfloat16)
    packed = jnp.concatenate(
        [up_cast[:, :MAIN], down_cast[:, :MAIN], up_cast[:, MAIN:], down_cast[:, MAIN:], spare],
        axis=1,
    )
    down_probe_t = down_probe.T

    few = width // N_Z
    goal = jnp.concatenate(
        [
            lax.dynamic_slice_in_dim(
                targets, place(z // 2, z % 2, k) * own_rows, own_rows, 1
            ).T
            for k in (0, 1)
        ],
        axis=0,
    ).astype(jnp.float32)

    thin = jax.ShapeDtypeStruct((rows, hidden), jnp.float32)
    pair = jax.ShapeDtypeStruct((2 * rows, hidden), jnp.bfloat16)
    step_flops = 2 * rows * width * hidden
    blocks = jax.ShapeDtypeStruct((N_DP, rows, own_rows), jnp.bfloat16)
    normed, preact_dir = call(
        dir_kernel, "dir", [blocks, thin], step_flops, tokens, norm_gain[None], up_probe
    )
    weights, (normed, preact_dir) = gather_chips(packed, True, True, (normed, preact_dir))
    partial, acts, slopes, cross = call(
        forward_kernel,
        "forward",
        [jax.ShapeDtypeStruct((width, 2 * rows), jnp.bfloat16), pair, thin, thin],
        4 * step_flops,
        order,
        down_probe_t,
        normed,
        preact_dir,
        *weights,
    )
    scattered = lax.psum_scatter(partial, "z", scatter_dimension=0, tiled=True)

    acts_pair = jnp.concatenate([acts, from_along(acts, "core", 1)], axis=0)
    acts_all, _ = gather_chips(acts_pair, False, False)
    scattered, *acts_all = lax.optimization_barrier((scattered, *acts_all))

    other = lax.ppermute(scattered, "xhi", ((0, 1), (1, 0)))
    total = scattered.astype(jnp.float32) + other.astype(jnp.float32)
    less = jnp.concatenate([goal, jnp.zeros_like(goal)], axis=1)
    own_res = ((total - less) / tokens_all).astype(jnp.bfloat16)
    res_both = lax.all_gather(own_res, "z", axis=0, tiled=True)

    moved = []
    for k in (0, 1):
        pairs = [
            (
                (((yy * 2 + xx) * 2) + cc) * N_Z + zz,
                ((((yy + zz // 2) % N_Y * 2) + (xx + zz) % 2) * 2 + (cc + k) % 2) * N_Z + zz,
            )
            for yy in range(N_Y)
            for xx in range(2)
            for cc in range(2)
            for zz in range(N_Z)
        ]
        piece = own_res[k * own_rows : (k + 1) * own_rows]
        moved.append(lax.ppermute(piece, (*DP, "z"), pairs))
    normed_t = after(normed, own_res).swapaxes(1, 2)
    inputs = lax.all_to_all(normed_t, DP, 0, 0, tiled=True)
    moved_both = jnp.stack(moved)
    res_both, inputs, moved_both = lax.optimization_barrier((res_both, inputs, moved_both))
    res_all = lax.all_gather(moved_both, "z", axis=0, tiled=True)

    grads = call(
        backward_kernel,
        "backward",
        jax.ShapeDtypeStruct((2 * rows + EXTRA, hidden), jnp.bfloat16),
        3 * step_flops,
        order,
        down_probe_t,
        res_both,
        slopes,
        cross,
        *weights,
    )
    grads_all, _ = gather_chips(grads, True, False)

    wide = jax.ShapeDtypeStruct((own_rows, hidden), jnp.float32)
    tile = jax.ShapeDtypeStruct((8, LANES), jnp.float32)
    up_grad, up_hess, loss = call(
        up_kernel,
        "up_products",
        [wide, wide, tile],
        2 * step_flops,
        order,
        inputs,
        *grads_all,
        scratch=(pltpu.VMEM((N_DP, 8, LANES), jnp.float32),),
    )
    down_grad, down_hess = call(
        down_kernel, "down_products", [wide, wide], 3 * step_flops, res_all, *acts_all
    )

    own = index[None]
    up_hut = jnp.abs(signs_of(up_probe, own).astype(jnp.float32) * up_hess)
    spot = lax.broadcasted_iota(jnp.int32, (hidden, hidden), 0) // BLOCK
    spread = lax.broadcasted_iota(jnp.int32, (hidden, hidden), 1) // BLOCK
    average = jnp.where(spot == spread, 1.0 / BLOCK, 0.0).astype(jnp.float32)
    up_diag = jnp.dot(up_hut, average, precision=lax.Precision.HIGHEST)
    down_hut = jnp.abs(signs_of(down_probe_t, own).astype(jnp.float32) * down_hess)
    means = jnp.mean(down_hut.reshape(own_rows // BLOCK, BLOCK, hidden), axis=1)
    down_diag = jnp.repeat(means, BLOCK, axis=0)
    up_out = stepped(up_grad, up_diag, up_first, up_second)
    down_out = stepped(down_grad, down_diag, down_first.T, down_second.T)
    return (loss[0, 0], *up_out, *(v.T for v in down_out))


def solution(mesh):
    fine = Mesh(mesh.devices.reshape(N_Y, 2, 2, N_Z, 2), (*DP, *FS))
    placed = (
        P(DP, None),
        P(DP, None),
        P(),
        P(DP, FS),
        P(FS, DP),
        P(None, FS),
        P(FS, None),
        P(DP, FS),
        P(DP, FS),
        P(FS, DP),
        P(FS, DP),
    )
    return jax.shard_map(
        local,
        mesh=fine,
        in_specs=placed,
        out_specs=(P(), P(DP, FS), P(DP, FS), P(DP, FS), P(FS, DP), P(FS, DP), P(FS, DP)),
        check_vma=False,
    )
```

```python
import jax
import jax.numpy as jnp
from jax import lax
from jax.experimental import pallas as pl
from jax.experimental.pallas import tpu as pltpu
from jax.sharding import Mesh, PartitionSpec as P


BLOCK = 16
STEP = 10
N_Z = 8
N_Y = 4
N_DP = 16

norm_eps = 1e-05
beta_one = 0.9
beta_two = 0.999
adam_eps = 1e-08

DP = ("y", "xlo", "core")
FS = ("z", "xhi")
LANES = 128
MAIN = 384
EXTRA = 32


def dot_first(left, right):
    return lax.dot_general(
        left, right, (((0,), (0,)), ((), ())), preferred_element_type=jnp.float32
    )


def dot_plain(left, right):
    return jnp.dot(left, right, preferred_element_type=jnp.float32)


def from_along(value, axis, step):
    size = lax.axis_size(axis)
    return lax.ppermute(value, axis, [(s, (s - step) % size) for s in range(size)])


def fenced(values):
    return list(lax.optimization_barrier(tuple(values)))


def gather_chips(shard, swap, split, early=(), also=()):
    half = shard.shape[0] // 2
    parts = {(0, 0): [shard]}
    others = {}

    def cross(*steps):
        if swap:
            held = [p for step in steps for p in parts[step]]
            joined = jnp.concatenate(held, axis=0) if len(held) > 1 else held[0]
            got = from_along(joined, "core", 1)
            rows = shard.shape[0]
            for k, step in enumerate(steps):
                others[step] = [got[k * rows : (k + 1) * rows]]

    def arrive(steps, extra=()):
        held = [(table, step) for step in steps for table in (parts, others) if step in table]
        lens = [len(table[step]) for table, step in held]
        values = fenced([p for table, step in held for p in table[step]] + list(extra))
        for (table, step), n in zip(held, lens):
            table[step], values = values[:n], values[n:]
        return values

    cross((0, 0))
    parts[3, 0] = [from_along(shard, "y", -1)]
    parts[1, 0] = [from_along(shard, "y", 1)]
    parts[0, 1] = [from_along(shard, "xlo", 1)]
    early = arrive([(3, 0), (1, 0), (0, 1)], early)
    cross((3, 0), (1, 0), (0, 1))
    parts[2, 0] = [from_along(parts[1, 0][0], "y", 1)]
    parts[3, 1] = [from_along(parts[0, 1][0], "y", -1)]
    parts[1, 1] = [from_along(parts[1, 0][0], "xlo", 1)]
    also = arrive([(2, 0), (3, 1), (1, 1), (3, 0), (1, 0), (0, 1)], also)
    if split:
        parts[2, 1] = [
            from_along(parts[2, 0][0][:half], "xlo", 1),
            from_along(parts[1, 1][0][half:], "y", 1),
        ]
    else:
        parts[2, 1] = [from_along(parts[2, 0][0], "xlo", 1)]
    cross((2, 0), (3, 1), (1, 1))
    arrive([(2, 1)])
    cross((2, 1))
    if swap:
        parts = {(*k, dc): t[k] for dc, t in enumerate((parts, others)) for k in t}
    return [p for step in sorted(parts) for p in parts[step]], early, also


def to_owner(piece, k):
    pairs = [
        (
            (((yy * 2 + xx) * 2) + cc) * N_Z + zz,
            ((((yy + zz // 2) % N_Y * 2) + (xx + zz) % 2) * 2 + (cc + k) % 2) * N_Z + zz,
        )
        for yy in range(N_Y)
        for xx in range(2)
        for cc in range(2)
        for zz in range(N_Z)
    ]
    return lax.ppermute(piece, (*DP, "z"), pairs)


STEPS = [(dy, dx, dc) for dy in range(N_Y) for dx in range(2) for dc in range(2)]


def fetch(refs, store_ref, sems, split=False):
    refs = list(refs)
    per_chip = store_ref.shape[0] // (N_DP // 2)
    for r in range(store_ref.shape[0]):
        if split and r == 5 * per_chip:
            half = store_ref.shape[1] // 2
            for k in (0, 1):
                target = store_ref.at[r, pl.ds(k * half, half)]
                pltpu.make_async_copy(refs.pop(0), target, sems.at[r]).start()
        else:
            pltpu.make_async_copy(refs.pop(0), store_ref.at[r], sems.at[r]).start()


def arrived(store_ref, sems, r):
    pltpu.make_async_copy(store_ref.at[r], store_ref.at[r], sems.at[r]).wait()


def last_last(left, right):
    return lax.dot_general(
        left, right, (((1,), (1,)), ((), ())), preferred_element_type=jnp.float32
    )


def block_signs(words, block):
    halves = [1 - 2 * ((words >> (2 * block + h)) & 1) for h in (0, 1)]
    return jnp.concatenate(halves, axis=0).astype(jnp.float32).astype(jnp.bfloat16)


def dir_kernel(tokens_ref, gain_ref, probe_ref, normed_ref, out_ref):
    values = tokens_ref[...].astype(jnp.float32)
    scale = lax.rsqrt(jnp.mean(values * values, axis=1, keepdims=True) + norm_eps)
    own = normed_ref.shape[2]
    words = probe_ref[...]
    out_ref[...] = jnp.zeros_like(out_ref)

    def step(p, carry):
        at = pl.ds(pl.multiple_of(p * 2 * own, LANES), 2 * own)
        normed = tokens_ref[:, at].astype(jnp.float32) * scale * gain_ref[:, at]
        for k in (0, 1):
            block = normed[:, k * own : (k + 1) * own].astype(jnp.bfloat16)
            normed_ref[2 * p + k] = block
            out_ref[...] += dot_plain(block, block_signs(words, 2 * p + k))
        return carry

    lax.fori_loop(0, N_DP // 2, step, 0)


def forward_kernel(order_ref, probe_ref, normed_ref, dir_ref, *refs):
    piece_refs, refs = refs[:-7], refs[-7:]
    part_ref, acts_ref, slopes_ref, cross_ref, store_ref, pre_ref, sems = refs
    fetch(piece_refs, store_ref, sems, True)
    rows, hidden = dir_ref.shape
    rest = hidden - MAIN
    pre_ref[...] = jnp.zeros_like(pre_ref)

    def up_step(r, carry):
        arrived(store_ref, sems, r)
        up = jnp.concatenate([store_ref[r, :, :MAIN], store_ref[r, :, 2 * MAIN :]], axis=1)
        pre_ref[...] += dot_plain(normed_ref[order_ref[r]], up)
        return carry

    lax.fori_loop(0, N_DP, up_step, 0)
    preact = pre_ref[:, :hidden]
    preact_dir = dir_ref[...]
    logistic = jax.nn.sigmoid(preact)
    active = (preact * logistic).astype(jnp.bfloat16)
    slopes = logistic * (1.0 + preact * (1.0 - logistic))
    curves = logistic * (1.0 - logistic) * (2.0 + preact * (1.0 - 2.0 * logistic))
    active_dir = (slopes * preact_dir).astype(jnp.bfloat16)
    slopes_ref[...] = slopes
    cross_ref[...] = curves * preact_dir
    acts_ref[:rows] = active_dir
    acts_ref[rows:] = active
    lead = jnp.concatenate([active, active_dir], axis=0)
    lead = jnp.concatenate(
        [
            lead[:, :MAIN],
            jnp.zeros((2 * rows, rest), jnp.bfloat16),
            lead[:, MAIN:],
            jnp.zeros((2 * rows, LANES - 2 * rest), jnp.bfloat16),
        ],
        axis=1,
    )
    words = probe_ref[...]
    own = store_ref.shape[1]

    def down_step(r, carry):
        out = last_last(store_ref[r, :, MAIN:], lead)
        side = last_last(block_signs(words, order_ref[r]), active)
        at = pl.ds(pl.multiple_of(r * own, own), own)
        part_ref[at, :rows] = out[:, :rows].astype(jnp.bfloat16)
        part_ref[at, rows:] = (out[:, rows:] + side).astype(jnp.bfloat16)
        return carry

    lax.fori_loop(0, N_DP, down_step, 0)


def backward_kernel(order_ref, probe_ref, res_ref, slopes_ref, cross_ref, *refs):
    piece_refs, (out_ref, store_ref, main_ref, side_ref, square_ref, sems) = refs[:-6], refs[-6:]
    fetch(piece_refs, store_ref, sems, True)
    words = probe_ref[...]
    own = store_ref.shape[1]
    rows, hidden = slopes_ref.shape
    for ref in (main_ref, side_ref, square_ref):
        ref[...] = jnp.zeros_like(ref)

    def step(r, carry):
        arrived(store_ref, sems, r)
        res = res_ref[pl.ds(pl.multiple_of(r * own, own), own), :]
        residual = res[:, :rows].astype(jnp.float32)
        square_ref[...] += jnp.sum(residual * residual, axis=0, keepdims=True)
        main_ref[...] += dot_first(res, store_ref[r, :, MAIN:])
        side_ref[...] += dot_first(res[:, :rows], block_signs(words, order_ref[r]))
        return carry

    lax.fori_loop(0, N_DP, step, 0)
    rest = hidden - MAIN
    both = jnp.concatenate([main_ref[:, :MAIN], main_ref[:, hidden : hidden + rest]], axis=1)
    grad_active = both[:rows]
    hess_active = both[rows:] + side_ref[...]
    slopes = slopes_ref[...]
    out_ref[:rows] = (slopes * grad_active).astype(jnp.bfloat16)
    hess = cross_ref[...] * grad_active + slopes * hess_active
    out_ref[rows : 2 * rows] = hess.astype(jnp.bfloat16)
    loss = jnp.sum(square_ref[...], axis=1, keepdims=True) * (0.5 * rows * N_DP)
    high = loss.astype(jnp.bfloat16).astype(jnp.float32)
    lane = lax.broadcasted_iota(jnp.int32, (EXTRA, hidden), 1)
    parts = jnp.where(lane == 0, high, jnp.where(lane == 1, loss - high, 0.0))
    out_ref[2 * rows :] = parts.astype(jnp.bfloat16)


def stepped(grad, diag, first, second, out_refs):
    first_new = beta_one * first + (1.0 - beta_one) * grad
    second_new = beta_two * second + (1.0 - beta_two) * diag * diag
    out_refs[0][...] = first_new
    out_refs[1][...] = second_new
    out_refs[2][...] = (
        first_new
        / (1.0 - beta_one**STEP)
        / (jnp.sqrt(second_new / (1.0 - beta_two**STEP)) + adam_eps)
    )


def own_hut(probe_ref, order_ref, hess_ref):
    signs = block_signs(probe_ref[...], order_ref[0]).astype(jnp.float32)
    return jnp.abs(signs * hess_ref[...])


def down_kernel(order_ref, probe_ref, first_ref, second_ref, res_ref, *refs):
    piece_refs, refs = refs[:-7], refs[-7:]
    out_refs, (store_ref, grad_ref, hess_ref, sems) = refs[:3], refs[3:]
    fetch(piece_refs, store_ref, sems)
    tok = res_ref.shape[2] // 2
    grad_ref[...] = jnp.zeros_like(grad_ref)
    hess_ref[...] = jnp.zeros_like(hess_ref)

    def step(chip, carry):
        base = (lax.rem(N_Y - chip // 2, N_Y) * 2 + lax.rem(chip, 2)) * 2
        arrived(store_ref, sems, chip)
        acts = store_ref[chip]
        res = [res_ref[base + k] for k in (0, 1)]
        hess_ref[...] += dot_plain(jnp.concatenate(res, axis=1), acts)
        act = [acts[q + tok : q + 2 * tok] for q in (0, 2 * tok)]
        left = jnp.concatenate([v[:, :tok] for v in res], axis=1)
        grad_ref[...] += dot_plain(left, jnp.concatenate(act, axis=0))
        return carry

    lax.fori_loop(0, N_DP // 2, step, 0)
    hut = own_hut(probe_ref, order_ref, hess_ref)
    own, hidden = hut.shape
    means = jnp.mean(hut.reshape(own // BLOCK, BLOCK, hidden), axis=1, keepdims=True)
    diag = jnp.broadcast_to(means, (own // BLOCK, BLOCK, hidden)).reshape(own, hidden)
    stepped(grad_ref[...], diag, first_ref[...], second_ref[...], out_refs)


def up_kernel(order_ref, probe_ref, first_ref, second_ref, in_ref, *refs):
    piece_refs, refs = refs[:-9], refs[-9:]
    out_refs, (loss_ref, store_ref, grad_ref, hess_ref, sums_ref, sems) = refs[:3], refs[3:]
    fetch(piece_refs, store_ref, sems)
    tok = in_ref.shape[2]
    grad_ref[...] = jnp.zeros_like(grad_ref)
    hess_ref[...] = jnp.zeros_like(hess_ref)

    def step(dy, carry):
        some = [4 * dy + k for k in range(4)]
        for r in some:
            arrived(store_ref, sems, r)
        base = lax.rem(N_Y - dy, N_Y) * 4
        left = jnp.concatenate([in_ref[base + k] for k in range(4)], axis=1)
        right = [jnp.concatenate([store_ref[r, q : q + tok] for r in some]) for q in (0, tok)]
        grad_ref[...] += dot_plain(left, right[0])
        hess_ref[...] += dot_plain(left, right[1])
        for r in some:
            losses = store_ref[r, 2 * tok :, :LANES].astype(jnp.float32)
            sums_ref[order_ref[r]] = losses[:8]
        return carry

    lax.fori_loop(0, N_Y, step, 0)
    total = sums_ref[0]
    for s in range(1, N_DP):
        total += sums_ref[s]
    loss_ref[...] = jnp.broadcast_to(total[:, 0:1] + total[:, 1:2], loss_ref.shape)
    hut = own_hut(probe_ref, order_ref, hess_ref)
    hidden = hut.shape[1]
    spot = lax.broadcasted_iota(jnp.int32, (hidden, hidden), 0) // BLOCK
    spread = lax.broadcasted_iota(jnp.int32, (hidden, hidden), 1) // BLOCK
    same = jnp.where(spot == spread, 1.0, 0.0).astype(jnp.bfloat16)
    high = hut.astype(jnp.bfloat16)
    low = (hut - high.astype(jnp.float32)).astype(jnp.bfloat16)
    diag = (dot_plain(high, same) + dot_plain(low, same)) * (1.0 / BLOCK)
    stepped(grad_ref[...], diag, first_ref[...], second_ref[...], out_refs)


def call(kernel, name, outs, flops, *operands, pieces=(), scratch=()):
    in_specs = [
        pl.BlockSpec(memory_space=pltpu.SMEM if o.ndim == 1 else pltpu.VMEM) for o in operands
    ]
    in_specs += [pl.BlockSpec(memory_space=pl.ANY) for _ in pieces]
    operands = (*operands, *pieces)
    return pl.pallas_call(
        kernel,
        in_specs=in_specs,
        out_specs=jax.tree.map(lambda _: pl.BlockSpec(memory_space=pltpu.VMEM), outs),
        out_shape=outs,
        scratch_shapes=scratch,
        name=name,
        cost_estimate=pl.CostEstimate(
            flops=flops,
            bytes_accessed=sum(o.size * o.dtype.itemsize for o in operands),
            transcendentals=0,
        ),
    )(*operands)


def local(
    tokens,
    targets,
    norm_gain,
    up_master,
    down_master,
    up_probe,
    down_probe,
    up_first,
    up_second,
    down_first,
    down_second,
):
    rows, width = tokens.shape
    own_rows, hidden = up_master.shape
    tokens_all = jnp.float32(rows * lax.axis_size(DP))
    index = lax.axis_index(DP)
    z = lax.axis_index("z")
    y, x, c = (lax.axis_index(a) for a in DP)
    place = lambda dy, dx, dc: (((y + dy) % N_Y) * 2 + (x + dx) % 2) * 2 + (c + dc) % 2
    order = jnp.stack([place(*step) for step in STEPS]).astype(jnp.int32)

    up_cast = up_master.astype(jnp.bfloat16)
    down_cast = down_master.T.astype(jnp.bfloat16)
    spare = jnp.zeros((own_rows, LANES - 2 * (hidden - MAIN)), jnp.bfloat16)
    packed = jnp.concatenate(
        [up_cast[:, :MAIN], down_cast[:, :MAIN], up_cast[:, MAIN:], down_cast[:, MAIN:], spare],
        axis=1,
    )
    down_probe_t = down_probe.T

    few = width // N_Z
    goal = jnp.concatenate(
        [
            lax.dynamic_slice_in_dim(
                targets, place(z // 2, z % 2, k) * own_rows, own_rows, 1
            ).T
            for k in (0, 1)
        ],
        axis=0,
    ).astype(jnp.float32)

    thin = jax.ShapeDtypeStruct((rows, hidden), jnp.float32)
    pair = jax.ShapeDtypeStruct((2 * rows, hidden), jnp.bfloat16)
    step_flops = 2 * rows * width * hidden
    stored = pltpu.VMEM((N_DP, own_rows, packed.shape[1]), jnp.bfloat16)
    in_blocks = pltpu.SemaphoreType.DMA((N_DP,))
    blocks = jax.ShapeDtypeStruct((N_DP, rows, own_rows), jnp.bfloat16)
    normed, preact_dir = call(
        dir_kernel, "dir", [blocks, thin], step_flops, tokens, norm_gain[None], up_probe
    )
    weights, (normed_soon,), (normed, preact_dir) = gather_chips(
        packed, True, True, (normed,), (normed, preact_dir)
    )
    moved = [
        to_owner(lax.dynamic_index_in_dim(normed_soon, place(z // 2, z % 2, k), 0, False).T, k)
        for k in (0, 1)
    ]
    inputs = lax.all_gather(jnp.stack(moved), "z", axis=0, tiled=True)
    partial, acts, slopes, cross = call(
        forward_kernel,
        "forward",
        [jax.ShapeDtypeStruct((width, 2 * rows), jnp.bfloat16), pair, thin, thin],
        4 * step_flops,
        order,
        down_probe_t,
        normed,
        preact_dir,
        pieces=weights,
        scratch=[stored, pltpu.VMEM((rows, MAIN + LANES), jnp.float32), in_blocks],
    )
    partial, inputs = fenced((partial, inputs))
    scattered = lax.psum_scatter(partial, "z", scatter_dimension=0, tiled=True)

    acts_pair = jnp.concatenate([acts, from_along(acts, "core", 1)], axis=0)
    acts_all, _, _ = gather_chips(acts_pair, False, False)
    scattered, *acts_all = lax.optimization_barrier((scattered, *acts_all))

    other = lax.ppermute(scattered, "xhi", ((0, 1), (1, 0)))
    total = scattered.astype(jnp.float32) + other.astype(jnp.float32)
    less = jnp.concatenate([goal, jnp.zeros_like(goal)], axis=1)
    own_res = ((total - less) / tokens_all).astype(jnp.bfloat16)
    res_both = lax.all_gather(own_res, "z", axis=0, tiled=True)

    moved = [to_owner(own_res[k * own_rows : (k + 1) * own_rows], k) for k in (0, 1)]
    res_both, moved_both = fenced((res_both, jnp.stack(moved)))
    res_all = lax.all_gather(moved_both, "z", axis=0, tiled=True)

    grads = call(
        backward_kernel,
        "backward",
        jax.ShapeDtypeStruct((2 * rows + EXTRA, hidden), jnp.bfloat16),
        3 * step_flops,
        order,
        down_probe_t,
        res_both,
        slopes,
        cross,
        pieces=weights,
        scratch=[
            stored,
            pltpu.VMEM((2 * rows, MAIN + LANES), jnp.float32),
            pltpu.VMEM((rows, hidden), jnp.float32),
            pltpu.VMEM((1, rows), jnp.float32),
            in_blocks,
        ],
    )
    grads_all, _, _ = gather_chips(grads, True, False)

    wide = jax.ShapeDtypeStruct((own_rows, hidden), jnp.float32)
    tile = jax.ShapeDtypeStruct((8, LANES), jnp.float32)
    sums = [pltpu.VMEM(wide.shape, jnp.float32)] * 2
    *up_out, loss = call(
        up_kernel,
        "up_products",
        [wide, wide, wide, tile],
        2 * step_flops,
        order,
        up_probe,
        up_first,
        up_second,
        inputs,
        pieces=grads_all,
        scratch=[
            pltpu.VMEM((N_DP, *grads.shape), jnp.bfloat16),
            *sums,
            pltpu.VMEM((N_DP, *tile.shape), jnp.float32),
            in_blocks,
        ],
    )
    down_out = call(
        down_kernel,
        "down_products",
        [wide, wide, wide],
        3 * step_flops,
        order,
        down_probe_t,
        down_first.T,
        down_second.T,
        res_all,
        pieces=acts_all,
        scratch=[
            pltpu.VMEM((N_DP // 2, *acts_pair.shape), jnp.bfloat16),
            *sums,
            pltpu.SemaphoreType.DMA((N_DP // 2,)),
        ],
    )
    return (loss[0, 0], *up_out, *(v.T for v in down_out))


def solution(mesh):
    fine = Mesh(mesh.devices.reshape(N_Y, 2, 2, N_Z, 2), (*DP, *FS))
    placed = (
        P(DP, None),
        P(DP, None),
        P(),
        P(DP, FS),
        P(FS, DP),
        P(None, FS),
        P(FS, None),
        P(DP, FS),
        P(DP, FS),
        P(FS, DP),
        P(FS, DP),
    )
    return jax.shard_map(
        local,
        mesh=fine,
        in_specs=placed,
        out_specs=(P(), P(DP, FS), P(DP, FS), P(DP, FS), P(FS, DP), P(FS, DP), P(FS, DP)),
        check_vma=False,
    )
```

```python
import functools

import jax
import jax.numpy as jnp
from jax import lax
from jax.experimental import pallas as pl
from jax.experimental.pallas import tpu as pltpu
from jax.sharding import Mesh, PartitionSpec as P


BLOCK = 16
STEP = 10
N_Z = 8
N_Y = 4
N_DP = 16

norm_eps = 1e-05
beta_one = 0.9
beta_two = 0.999
adam_eps = 1e-08

DP = ("y", "xlo", "core")
FS = ("z", "xhi")
LANES = 128
MAIN = 384
EXTRA = 32


def dot_first(left, right):
    return lax.dot_general(
        left, right, (((0,), (0,)), ((), ())), preferred_element_type=jnp.float32
    )


def dot_plain(left, right):
    return jnp.dot(left, right, preferred_element_type=jnp.float32)


def after(value, *others):
    return lax.optimization_barrier((value, *others))[0]


def from_along(value, axis, step):
    size = lax.axis_size(axis)
    return lax.ppermute(value, axis, [(s, (s - step) % size) for s in range(size)])


def fenced(values):
    return list(lax.optimization_barrier(tuple(values)))


def gather_chips(shard, swap, split, group=False, also=()):
    half = shard.shape[0] // 2
    parts = {(0, 0): [shard]}
    others = {}
    joint = {}

    def cross(*steps):
        if group:
            held = [p for step in steps for p in parts[step]]
            joined = jnp.concatenate(held, axis=0) if len(held) > 1 else held[0]
            got = from_along(joined, "core", 1)
            for k, step in enumerate(steps):
                joint[step] = [(got, k * shard.shape[0])]
        elif swap:
            for step in steps:
                full = parts[step]
                full = jnp.concatenate(full, axis=0) if len(full) > 1 else full[0]
                others[step] = [from_along(full, "core", 1)]

    def arrive(steps, extra=()):
        held = [(table, step) for step in steps for table in (parts, others) if step in table]
        lens = [len(table[step]) for table, step in held]
        values = fenced([p for table, step in held for p in table[step]] + list(extra))
        for (table, step), n in zip(held, lens):
            table[step], values = values[:n], values[n:]
        return values

    cross((0, 0))
    parts[3, 0] = [from_along(shard, "y", -1)]
    parts[1, 0] = [from_along(shard, "y", 1)]
    parts[0, 1] = [from_along(shard, "xlo", 1)]
    arrive([(3, 0), (1, 0), (0, 1)])
    cross((3, 0), (1, 0), (0, 1))
    parts[2, 0] = [from_along(parts[1, 0][0], "y", 1)]
    parts[3, 1] = [from_along(parts[0, 1][0], "y", -1)]
    parts[1, 1] = [from_along(parts[1, 0][0], "xlo", 1)]
    also = arrive([(2, 0), (3, 1), (1, 1), (3, 0), (1, 0), (0, 1)], also)
    if split:
        parts[2, 1] = [
            from_along(parts[2, 0][0][:half], "xlo", 1),
            from_along(parts[1, 1][0][half:], "y", 1),
        ]
    else:
        parts[2, 1] = [from_along(parts[2, 0][0], "xlo", 1)]
    cross((2, 0), (3, 1), (1, 1))
    arrive([(2, 1)])
    cross((2, 1))
    if swap:
        parts = {(*k, dc): t[k] for dc, t in enumerate((parts, joint or others)) for k in t}
    return [p for step in sorted(parts) for p in parts[step]], also


STEPS = [(dy, dx, dc) for dy in range(N_Y) for dx in range(2) for dc in range(2)]


def fetch(refs, plan, store_ref, sems, split=False):
    plan = list(plan)
    per_chip = store_ref.shape[0] // (N_DP // 2)
    whole = store_ref.shape[1]
    for r in range(store_ref.shape[0]):
        count = 2 if split and r == 5 * per_chip else 1
        rows = whole // count
        for k in range(count):
            which, row = plan.pop(0)
            target = store_ref.at[r, pl.ds(k * rows, rows)] if count > 1 else store_ref.at[r]
            source = refs[which]
            if source.shape[0] != rows:
                source = source.at[pl.ds(row, rows)]
            pltpu.make_async_copy(source, target, sems.at[r]).start()


def arrived(store_ref, sems, r):
    pltpu.make_async_copy(store_ref.at[r], store_ref.at[r], sems.at[r]).wait()


def last_last(left, right):
    return lax.dot_general(
        left, right, (((1,), (1,)), ((), ())), preferred_element_type=jnp.float32
    )


def block_signs(words, block):
    halves = [1 - 2 * ((words >> (2 * block + h)) & 1) for h in (0, 1)]
    return jnp.concatenate(halves, axis=0).astype(jnp.float32).astype(jnp.bfloat16)


def dir_kernel(tokens_ref, gain_ref, probe_ref, normed_ref, out_ref):
    values = tokens_ref[...].astype(jnp.float32)
    scale = lax.rsqrt(jnp.mean(values * values, axis=1, keepdims=True) + norm_eps)
    own = normed_ref.shape[2]
    words = probe_ref[...]
    out_ref[...] = jnp.zeros_like(out_ref)

    def step(p, carry):
        at = pl.ds(pl.multiple_of(p * 2 * own, LANES), 2 * own)
        normed = tokens_ref[:, at].astype(jnp.float32) * scale * gain_ref[:, at]
        for k in (0, 1):
            block = normed[:, k * own : (k + 1) * own].astype(jnp.bfloat16)
            normed_ref[2 * p + k] = block
            out_ref[...] += dot_plain(block, block_signs(words, 2 * p + k))
        return carry

    lax.fori_loop(0, N_DP // 2, step, 0)


def forward_kernel(plan, order_ref, probe_ref, normed_ref, dir_ref, *refs):
    piece_refs, refs = refs[:-7], refs[-7:]
    part_ref, acts_ref, slopes_ref, cross_ref, store_ref, pre_ref, sems = refs
    fetch(piece_refs, plan, store_ref, sems, True)
    rows, hidden = dir_ref.shape
    rest = hidden - MAIN
    pre_ref[...] = jnp.zeros_like(pre_ref)

    def up_step(r, carry):
        arrived(store_ref, sems, r)
        up = jnp.concatenate([store_ref[r, :, :MAIN], store_ref[r, :, 2 * MAIN :]], axis=1)
        pre_ref[...] += dot_plain(normed_ref[order_ref[r]], up)
        return carry

    lax.fori_loop(0, N_DP, up_step, 0)
    preact = pre_ref[:, :hidden]
    preact_dir = dir_ref[...]
    logistic = jax.nn.sigmoid(preact)
    active = (preact * logistic).astype(jnp.bfloat16)
    slopes = logistic * (1.0 + preact * (1.0 - logistic))
    curves = logistic * (1.0 - logistic) * (2.0 + preact * (1.0 - 2.0 * logistic))
    active_dir = (slopes * preact_dir).astype(jnp.bfloat16)
    slopes_ref[...] = slopes
    cross_ref[...] = curves * preact_dir
    acts_ref[:rows] = active_dir
    acts_ref[rows:] = active
    lead = jnp.concatenate([active, active_dir], axis=0)
    lead = jnp.concatenate(
        [
            lead[:, :MAIN],
            jnp.zeros((2 * rows, rest), jnp.bfloat16),
            lead[:, MAIN:],
            jnp.zeros((2 * rows, LANES - 2 * rest), jnp.bfloat16),
        ],
        axis=1,
    )
    words = probe_ref[...]
    own = store_ref.shape[1]

    def down_step(r, carry):
        out = last_last(store_ref[r, :, MAIN:], lead)
        side = last_last(block_signs(words, order_ref[r]), active)
        at = pl.ds(pl.multiple_of(r * own, own), own)
        part_ref[at, :rows] = out[:, :rows].astype(jnp.bfloat16)
        part_ref[at, rows:] = (out[:, rows:] + side).astype(jnp.bfloat16)
        return carry

    lax.fori_loop(0, N_DP, down_step, 0)


def backward_kernel(plan, order_ref, probe_ref, res_ref, slopes_ref, cross_ref, *refs):
    piece_refs, (out_ref, store_ref, main_ref, side_ref, square_ref, sems) = refs[:-6], refs[-6:]
    fetch(piece_refs, plan, store_ref, sems, True)
    words = probe_ref[...]
    own = store_ref.shape[1]
    rows, hidden = slopes_ref.shape
    for ref in (main_ref, side_ref, square_ref):
        ref[...] = jnp.zeros_like(ref)

    def step(r, carry):
        arrived(store_ref, sems, r)
        res = res_ref[pl.ds(pl.multiple_of(r * own, own), own), :]
        residual = res[:, :rows].astype(jnp.float32)
        square_ref[...] += jnp.sum(residual * residual, axis=0, keepdims=True)
        main_ref[...] += dot_first(res, store_ref[r, :, MAIN:])
        side_ref[...] += dot_first(res[:, :rows], block_signs(words, order_ref[r]))
        return carry

    lax.fori_loop(0, N_DP, step, 0)
    rest = hidden - MAIN
    both = jnp.concatenate([main_ref[:, :MAIN], main_ref[:, hidden : hidden + rest]], axis=1)
    grad_active = both[:rows]
    hess_active = both[rows:] + side_ref[...]
    slopes = slopes_ref[...]
    out_ref[:rows] = (slopes * grad_active).astype(jnp.bfloat16)
    hess = cross_ref[...] * grad_active + slopes * hess_active
    out_ref[rows : 2 * rows] = hess.astype(jnp.bfloat16)
    loss = jnp.sum(square_ref[...], axis=1, keepdims=True) * (0.5 * rows * N_DP)
    high = loss.astype(jnp.bfloat16).astype(jnp.float32)
    lane = lax.broadcasted_iota(jnp.int32, (EXTRA, hidden), 1)
    parts = jnp.where(lane == 0, high, jnp.where(lane == 1, loss - high, 0.0))
    out_ref[2 * rows :] = parts.astype(jnp.bfloat16)


def stepped(grad, diag, first, second, out_refs):
    first_new = beta_one * first + (1.0 - beta_one) * grad
    second_new = beta_two * second + (1.0 - beta_two) * diag * diag
    out_refs[0][...] = first_new
    out_refs[1][...] = second_new
    out_refs[2][...] = (
        first_new
        / (1.0 - beta_one**STEP)
        / (jnp.sqrt(second_new / (1.0 - beta_two**STEP)) + adam_eps)
    )


def own_hut(probe_ref, order_ref, hess_ref):
    signs = block_signs(probe_ref[...], order_ref[0]).astype(jnp.float32)
    return jnp.abs(signs * hess_ref[...])


def down_kernel(plan, order_ref, probe_ref, first_ref, second_ref, res_ref, *refs):
    piece_refs, refs = refs[:-7], refs[-7:]
    out_refs, (store_ref, grad_ref, hess_ref, sems) = refs[:3], refs[3:]
    fetch(piece_refs, plan, store_ref, sems)
    tok = res_ref.shape[2] // 2
    grad_ref[...] = jnp.zeros_like(grad_ref)
    hess_ref[...] = jnp.zeros_like(hess_ref)

    def step(chip, carry):
        base = (lax.rem(N_Y - chip // 2, N_Y) * 2 + lax.rem(chip, 2)) * 2
        arrived(store_ref, sems, chip)
        acts = store_ref[chip]
        res = [res_ref[base + k] for k in (0, 1)]
        hess_ref[...] += dot_plain(jnp.concatenate(res, axis=1), acts)
        act = [acts[q + tok : q + 2 * tok] for q in (0, 2 * tok)]
        left = jnp.concatenate([v[:, :tok] for v in res], axis=1)
        grad_ref[...] += dot_plain(left, jnp.concatenate(act, axis=0))
        return carry

    lax.fori_loop(0, N_DP // 2, step, 0)
    hut = own_hut(probe_ref, order_ref, hess_ref)
    own, hidden = hut.shape
    means = jnp.mean(hut.reshape(own // BLOCK, BLOCK, hidden), axis=1, keepdims=True)
    diag = jnp.broadcast_to(means, (own // BLOCK, BLOCK, hidden)).reshape(own, hidden)
    stepped(grad_ref[...], diag, first_ref[...], second_ref[...], out_refs)


def up_kernel(plan, order_ref, probe_ref, first_ref, second_ref, in_ref, *refs):
    piece_refs, refs = refs[:-9], refs[-9:]
    out_refs, (loss_ref, store_ref, grad_ref, hess_ref, sums_ref, sems) = refs[:3], refs[3:]
    fetch(piece_refs, plan, store_ref, sems)
    tok = in_ref.shape[2]
    grad_ref[...] = jnp.zeros_like(grad_ref)
    hess_ref[...] = jnp.zeros_like(hess_ref)

    def step(chip, carry):
        some = [2 * chip + k for k in range(2)]
        for r in some:
            arrived(store_ref, sems, r)
        left = jnp.concatenate([in_ref[order_ref[r]] for r in some], axis=1)
        right = [jnp.concatenate([store_ref[r, q : q + tok] for r in some]) for q in (0, tok)]
        grad_ref[...] += dot_plain(left, right[0])
        hess_ref[...] += dot_plain(left, right[1])
        for r in some:
            losses = store_ref[r, 2 * tok :, :LANES].astype(jnp.float32)
            sums_ref[order_ref[r]] = losses[:8]
        return carry

    lax.fori_loop(0, N_DP // 2, step, 0)
    total = sums_ref[0]
    for s in range(1, N_DP):
        total += sums_ref[s]
    loss_ref[...] = jnp.broadcast_to(total[:, 0:1] + total[:, 1:2], loss_ref.shape)
    hut = own_hut(probe_ref, order_ref, hess_ref)
    hidden = hut.shape[1]
    spot = lax.broadcasted_iota(jnp.int32, (hidden, hidden), 0) // BLOCK
    spread = lax.broadcasted_iota(jnp.int32, (hidden, hidden), 1) // BLOCK
    same = jnp.where(spot == spread, 1.0, 0.0).astype(jnp.bfloat16)
    high = hut.astype(jnp.bfloat16)
    low = (hut - high.astype(jnp.float32)).astype(jnp.bfloat16)
    diag = (dot_plain(high, same) + dot_plain(low, same)) * (1.0 / BLOCK)
    stepped(grad_ref[...], diag, first_ref[...], second_ref[...], out_refs)


def call(kernel, name, outs, flops, *operands, pieces=(), scratch=()):
    in_specs = [
        pl.BlockSpec(memory_space=pltpu.SMEM if o.ndim == 1 else pltpu.VMEM) for o in operands
    ]
    if pieces:
        pieces = [p if isinstance(p, tuple) else (p, 0) for p in pieces]
        arrays = []
        plan = []
        for array, row in pieces:
            known = [k for k, a in enumerate(arrays) if a is array]
            if not known:
                arrays.append(array)
            plan.append((known[0] if known else len(arrays) - 1, row))
        kernel = functools.partial(kernel, plan)
        in_specs += [pl.BlockSpec(memory_space=pl.ANY) for _ in arrays]
        operands = (*operands, *arrays)
    return pl.pallas_call(
        kernel,
        in_specs=in_specs,
        out_specs=jax.tree.map(lambda _: pl.BlockSpec(memory_space=pltpu.VMEM), outs),
        out_shape=outs,
        scratch_shapes=scratch,
        name=name,
        cost_estimate=pl.CostEstimate(
            flops=flops,
            bytes_accessed=sum(o.size * o.dtype.itemsize for o in operands),
            transcendentals=0,
        ),
    )(*operands)


def local(
    tokens,
    targets,
    norm_gain,
    up_master,
    down_master,
    up_probe,
    down_probe,
    up_first,
    up_second,
    down_first,
    down_second,
):
    rows, width = tokens.shape
    own_rows, hidden = up_master.shape
    tokens_all = jnp.float32(rows * lax.axis_size(DP))
    index = lax.axis_index(DP)
    z = lax.axis_index("z")
    y, x, c = (lax.axis_index(a) for a in DP)
    place = lambda dy, dx, dc: (((y + dy) % N_Y) * 2 + (x + dx) % 2) * 2 + (c + dc) % 2
    order = jnp.stack([place(*step) for step in STEPS]).astype(jnp.int32)

    up_cast = up_master.astype(jnp.bfloat16)
    down_cast = down_master.T.astype(jnp.bfloat16)
    spare = jnp.zeros((own_rows, LANES - 2 * (hidden - MAIN)), jnp.bfloat16)
    packed = jnp.concatenate(
        [up_cast[:, :MAIN], down_cast[:, :MAIN], up_cast[:, MAIN:], down_cast[:, MAIN:], spare],
        axis=1,
    )
    down_probe_t = down_probe.T

    few = width // N_Z
    goal = jnp.concatenate(
        [
            lax.dynamic_slice_in_dim(
                targets, place(z // 2, z % 2, k) * own_rows, own_rows, 1
            ).T
            for k in (0, 1)
        ],
        axis=0,
    ).astype(jnp.float32)

    thin = jax.ShapeDtypeStruct((rows, hidden), jnp.float32)
    pair = jax.ShapeDtypeStruct((2 * rows, hidden), jnp.bfloat16)
    step_flops = 2 * rows * width * hidden
    stored = pltpu.VMEM((N_DP, own_rows, packed.shape[1]), jnp.bfloat16)
    in_blocks = pltpu.SemaphoreType.DMA((N_DP,))
    blocks = jax.ShapeDtypeStruct((N_DP, rows, own_rows), jnp.bfloat16)
    normed, preact_dir = call(
        dir_kernel, "dir", [blocks, thin], step_flops, tokens, norm_gain[None], up_probe
    )
    weights, (normed, preact_dir) = gather_chips(packed, True, True, also=(normed, preact_dir))
    partial, acts, slopes, cross = call(
        forward_kernel,
        "forward",
        [jax.ShapeDtypeStruct((width, 2 * rows), jnp.bfloat16), pair, thin, thin],
        4 * step_flops,
        order,
        down_probe_t,
        normed,
        preact_dir,
        pieces=weights,
        scratch=[stored, pltpu.VMEM((rows, MAIN + LANES), jnp.float32), in_blocks],
    )
    scattered = lax.psum_scatter(partial, "z", scatter_dimension=0, tiled=True)

    acts_pair = jnp.concatenate([acts, from_along(acts, "core", 1)], axis=0)
    acts_all, _ = gather_chips(acts_pair, False, False)
    scattered, *acts_all = lax.optimization_barrier((scattered, *acts_all))

    other = lax.ppermute(scattered, "xhi", ((0, 1), (1, 0)))
    total = scattered.astype(jnp.float32) + other.astype(jnp.float32)
    less = jnp.concatenate([goal, jnp.zeros_like(goal)], axis=1)
    own_res = ((total - less) / tokens_all).astype(jnp.bfloat16)
    res_both = lax.all_gather(own_res, "z", axis=0, tiled=True)

    moved = []
    for k in (0, 1):
        pairs = [
            (
                (((yy * 2 + xx) * 2) + cc) * N_Z + zz,
                ((((yy + zz // 2) % N_Y * 2) + (xx + zz) % 2) * 2 + (cc + k) % 2) * N_Z + zz,
            )
            for yy in range(N_Y)
            for xx in range(2)
            for cc in range(2)
            for zz in range(N_Z)
        ]
        piece = own_res[k * own_rows : (k + 1) * own_rows]
        moved.append(lax.ppermute(piece, (*DP, "z"), pairs))
    normed_t = after(normed, own_res).swapaxes(1, 2)
    inputs = lax.all_to_all(normed_t, DP, 0, 0, tiled=True)
    moved_both = jnp.stack(moved)
    res_both, inputs, moved_both = lax.optimization_barrier((res_both, inputs, moved_both))
    res_all = lax.all_gather(moved_both, "z", axis=0, tiled=True)

    grads = call(
        backward_kernel,
        "backward",
        jax.ShapeDtypeStruct((2 * rows + EXTRA, hidden), jnp.bfloat16),
        3 * step_flops,
        order,
        down_probe_t,
        res_both,
        slopes,
        cross,
        pieces=weights,
        scratch=[
            stored,
            pltpu.VMEM((2 * rows, MAIN + LANES), jnp.float32),
            pltpu.VMEM((rows, hidden), jnp.float32),
            pltpu.VMEM((1, rows), jnp.float32),
            in_blocks,
        ],
    )
    grads_all, _ = gather_chips(grads, True, False, group=True)

    wide = jax.ShapeDtypeStruct((own_rows, hidden), jnp.float32)
    tile = jax.ShapeDtypeStruct((8, LANES), jnp.float32)
    sums = [pltpu.VMEM(wide.shape, jnp.float32)] * 2
    *up_out, loss = call(
        up_kernel,
        "up_products",
        [wide, wide, wide, tile],
        2 * step_flops,
        order,
        up_probe,
        up_first,
        up_second,
        inputs,
        pieces=grads_all,
        scratch=[
            pltpu.VMEM((N_DP, *grads.shape), jnp.bfloat16),
            *sums,
            pltpu.VMEM((N_DP, *tile.shape), jnp.float32),
            in_blocks,
        ],
    )
    down_out = call(
        down_kernel,
        "down_products",
        [wide, wide, wide],
        3 * step_flops,
        order,
        down_probe_t,
        down_first.T,
        down_second.T,
        res_all,
        pieces=acts_all,
        scratch=[
            pltpu.VMEM((N_DP // 2, *acts_pair.shape), jnp.bfloat16),
            *sums,
            pltpu.SemaphoreType.DMA((N_DP // 2,)),
        ],
    )
    return (loss[0, 0], *up_out, *(v.T for v in down_out))


def solution(mesh):
    fine = Mesh(mesh.devices.reshape(N_Y, 2, 2, N_Z, 2), (*DP, *FS))
    placed = (
        P(DP, None),
        P(DP, None),
        P(),
        P(DP, FS),
        P(FS, DP),
        P(None, FS),
        P(FS, None),
        P(DP, FS),
        P(DP, FS),
        P(FS, DP),
        P(FS, DP),
    )
    return jax.shard_map(
        local,
        mesh=fine,
        in_specs=placed,
        out_specs=(P(), P(DP, FS), P(DP, FS), P(DP, FS), P(FS, DP), P(FS, DP), P(FS, DP)),
        check_vma=False,
    )
```
